256 devices in a mesh: freq: 32 (over x, z), pts: 8 (over y, core).
Axes of the slice: x: 4, y: 4, z: 8, core: 2. Of those that a mesh axis runs over, the one named last changes fastest.
Arguments:
- snapshots: float32 [256, 5, 65536], P(None, None, ('pts', 'freq')), may hold values from -6 to 6
- weights: float32 [65536], P(('pts', 'freq')), may hold values from 0.25 to 4
- starts: int32 [3], replicated, may hold values from 0 to 128
- bins: int32 [64], replicated, may hold values from 0 to 63, each once
Outputs:
- modes: float32 [64, 2, 5, 65536], P('freq', None, None, 'pts')
- energy: float32 [64], P('freq')
The draws below stay inside these ranges and needn't reach their ends.
All inputs are finite; a program needn't handle non-finite values.
Results may differ from the reference program's by a relative error of at most 0.00024.
Values sent between devices are 32-bit elements; how exact they have to be, the bound alone decides.
No kernel may reach another device: no remote copies, remote signals or barrier semaphores. Data moves between devices by JAX's collectives and lax.ppermute only.
A program may use at most 64 MiB of HBM per device.

```python
import math
import jax
import jax.numpy as jnp
from jax import lax

NVAR = 5
NFFT = 128
NB = 3
ITERS = 8
KF = 64
NT = 256
NPTS = 65536


def block_scale(stream_key, dims, shards, least, largest):
    def one(dim, shards_of):
        steps = jax.random.uniform(jax.random.fold_in(jax.random.fold_in(stream_key, 6), dim), (shards_of,), jnp.float32, least / len(shards), largest / len(shards))
        return jnp.repeat(jnp.exp(steps), dims[dim] // shards_of).reshape((-1,) + (1,) * (len(dims) - dim - 1))

    loudness = one(*shards[0])
    for cut in shards[1:]:
        loudness = loudness * one(*cut)
    return loudness


def noise(stream_key, dims, deviation, limit, shards=(), kind=jnp.bfloat16):
    drawn = jax.random.normal(stream_key, dims, jnp.float32) * deviation
    if len(shards) > 0:
        drawn = block_scale(stream_key, dims, shards, -0.22, 0.18) * drawn
    return jnp.clip(drawn, min=-limit, max=limit).astype(kind)


def setup_inputs(seed: int = 0) -> dict:
    seeds = jax.random.split(jax.random.key(seed), 5)
    return {
        "snapshots": noise(seeds[0], (NT, NVAR, NPTS), 1.0, 6.0, ((2, 256),), jnp.float32),
        "weights": jnp.clip(jnp.exp(math.log(4.0) - 2.7725887 * jax.random.uniform(seeds[1], (NPTS,), jnp.float32) ** block_scale(seeds[1], (NPTS,), ((0, 256),), -0.2, 0.2)), 0.25, 4.0),
        "starts": jax.random.randint(seeds[2], (NB,), 0, NT - NFFT + 1).astype(jnp.int32),
        "bins": jax.random.permutation(seeds[3], KF).astype(jnp.int32),
    }


def dft_window():
    steps_t = jnp.arange(NFFT, dtype=jnp.float32)
    window = 0.5 - 0.5 * jnp.cos(2.0 * math.pi * steps_t / NFFT)
    return (window, 1.0 / jnp.sqrt(jnp.sum(window * window)))

def gram_of(spec, wts, count):
    weighted = spec * wts
    real_part = jnp.einsum('kacvp,kbcvp->kab', weighted, spec, precision=lax.Precision.HIGHEST)
    cross = jnp.einsum('kavp,kbvp->kab', weighted[:, :, 0], spec[:, :, 1], precision=lax.Precision.HIGHEST)
    return (real_part / count, (cross - jnp.swapaxes(cross, 1, 2)) / count)

def apply_gram(gram_re, gram_im, xr, xi):
    ur = lax.optimization_barrier(jnp.sum(gram_re * xr[:, None, :], 2)) - lax.optimization_barrier(jnp.sum(gram_im * xi[:, None, :], 2))
    ui = lax.optimization_barrier(jnp.sum(gram_re * xi[:, None, :], 2)) + lax.optimization_barrier(jnp.sum(gram_im * xr[:, None, :], 2))
    return (ur, ui)

def leading(gram_re, gram_im):
    xr = jnp.ones(gram_re.shape[:2], gram_re.dtype)
    xi = jnp.zeros(gram_re.shape[:2], gram_re.dtype)
    for step in range(ITERS):
        ur, ui = apply_gram(gram_re, gram_im, xr, xi)
        scale_now = jnp.sqrt(lax.optimization_barrier(jnp.sum(ur * ur + ui * ui, 1)))[:, None]
        xr, xi = (ur / scale_now, ui / scale_now)
    ur, ui = apply_gram(gram_re, gram_im, xr, xi)
    return (xr, xi, lax.optimization_barrier(jnp.sum(xr * ur + xi * ui, 1)))

def build_modes(spec, xr, xi, energy):
    hp = lax.Precision.HIGHEST
    real_part = jnp.einsum('kb,kbvp->kvp', xr, spec[:, :, 0], precision=hp) - jnp.einsum('kb,kbvp->kvp', xi, spec[:, :, 1], precision=hp)
    imag_part = jnp.einsum('kb,kbvp->kvp', xr, spec[:, :, 1], precision=hp) + jnp.einsum('kb,kbvp->kvp', xi, spec[:, :, 0], precision=hp)
    factor = 1.0 / jnp.sqrt(jnp.maximum(energy, 0.25))
    return jnp.stack([real_part, imag_part], 1) * factor[:, None, None, None]

def reference(snapshots, weights, starts, bins):
    centered = snapshots - lax.optimization_barrier(jnp.mean(snapshots, 0, keepdims=True))
    window, scale = dft_window()
    blocks = []
    for block in range(NB):
        segment = lax.dynamic_slice_in_dim(centered, starts[block].astype(jnp.int32), NFFT, 0)
        transformed = jnp.fft.rfft(segment * window[:, None, None], axis=0)[bins.astype(jnp.int32)]
        blocks.append(jnp.stack([jnp.real(transformed), jnp.imag(transformed)], 1) * scale)
    spec = jnp.stack(blocks, 1)
    gram_re, gram_im = gram_of(spec, weights, NPTS * NVAR)
    xr, xi, energy = leading(gram_re, gram_im)
    return (build_modes(spec, xr, xi, energy), energy)
```

```python
import math

import jax
import jax.numpy as jnp
from jax import lax
from jax.experimental import pallas as pl
from jax.experimental.pallas import tpu as pltpu
from jax.sharding import Mesh
from jax.sharding import PartitionSpec as P

NFFT = 128
NB = 3
ITERS = 8
KF = 64
LANES = 128
QS = 9
PAIRS = ((0, 1), (0, 2), (1, 2))
FREQ = ("freq_0", "freq_1")
PTS = ("pts_0", "pts_1")
PTS_FREQ = ("pts_0", "pts_1", "freq_0", "freq_1")
FIRST = ("freq_0", "pts_0")
SECOND = ("freq_1", "pts_1")


def halves(value):
    high = value.astype(jnp.bfloat16)
    return high, (value - high.astype(jnp.float32)).astype(jnp.bfloat16)


def product(a_high, a_low, b_high, b_low):
    def dot(a, b):
        return jnp.dot(a, b, preferred_element_type=jnp.float32)

    return dot(a_high, b_high) + dot(a_high, b_low) + dot(a_low, b_high)


def column(row, n):
    rows = lax.broadcasted_iota(jnp.int32, (n, n), 0)
    cols = lax.broadcasted_iota(jnp.int32, (n, n), 1)
    wide = jnp.broadcast_to(row, (n, n))
    return jnp.sum(jnp.where(rows == cols, wide, jnp.zeros_like(wide)), axis=1, keepdims=True)


def tables(starts_ref, bins, tab_ref):
    step = lax.broadcasted_iota(jnp.int32, (KF, NFFT), 1)
    angle = 2.0 * math.pi / NFFT
    scale = 1.0 / math.sqrt(sum((0.5 - 0.5 * math.cos(angle * t)) ** 2 for t in range(NFFT)))
    window = (0.5 - 0.5 * jnp.cos(step.astype(jnp.float32) * angle)) * scale
    slot_bins = column(bins.astype(jnp.float32), KF).astype(jnp.int32)
    phase = ((slot_bins * step) & (NFFT - 1)).astype(jnp.float32) * angle
    parts = (jnp.cos(phase) * window, -jnp.sin(phase) * window)
    zero = jnp.zeros((KF, NFFT), jnp.float32)
    for b in range(NB):
        start = starts_ref[b]
        for c in range(2):
            turned = pltpu.roll(parts[c], start & (NFFT - 1), 1)
            tab_ref[2 * b + c, :, :NFFT] = jnp.where(step >= start, turned, zero)
            tab_ref[2 * b + c, :, NFFT:] = jnp.where(step < start, turned, zero)


def spectra_kernel(
    starts_ref, bins_ref, wts_ref, x_hbm, gram_ref, high_ref, low_ref, tab_ref, x_ref, spec_ref,
    prod_ref, sems,
):
    n_var, n_time, n_pts = x_ref.shape
    copies = [pltpu.make_async_copy(x_hbm.at[v], x_ref.at[v], sems.at[v]) for v in range(n_var)]
    for copy in copies:
        copy.start()
    tables(starts_ref, bins_ref[...], tab_ref)
    t_high, t_low = halves(tab_ref[...].reshape(2 * NB * KF, n_time))
    for v in range(n_var):
        copies[v].wait()
        x = x_ref[v]
        high, low = halves(x - jnp.sum(x, axis=0, keepdims=True) * (1.0 / n_time))
        high_ref[v] = high
        low_ref[v] = low
        spec_ref[v] = product(t_high, t_low, high, low)

    def rows(tile, carry):
        first = pl.multiple_of(tile * 8, 8)
        totals = [None] * QS
        for lane in range(0, n_pts, LANES):
            sums = [None] * QS

            def put(q, value):
                sums[q] = value if sums[q] is None else sums[q] + value

            for v in range(n_var):
                s = [
                    spec_ref[v, pl.ds(KF * r + first, 8), lane : lane + LANES]
                    for r in range(2 * NB)
                ]
                re, im = s[0::2], s[1::2]
                for a in range(NB):
                    put(a, re[a] * re[a] + im[a] * im[a])
                for q, (a, c) in enumerate(PAIRS):
                    put(NB + q, re[a] * re[c] + im[a] * im[c])
                    put(2 * NB + q, re[a] * im[c] - im[a] * re[c])
            w = wts_ref[:, lane : lane + LANES]
            for q in range(QS):
                part = sums[q] * w
                totals[q] = part if totals[q] is None else totals[q] + part
        for q in range(QS):
            prod_ref[pl.ds(KF * q + first, 8), :] = totals[q]
        return carry

    lax.fori_loop(0, KF // 8, rows, 0)
    sums = lax.dot_general(
        jnp.ones((8, LANES), jnp.float32),
        prod_ref[...],
        (((1,), (1,)), ((), ())),
        precision=lax.Precision.HIGHEST,
        preferred_element_type=jnp.float32,
    )
    gram_ref[...] = jnp.broadcast_to(sums[0:1][None], gram_ref.shape)


def relay_kernel(in_ref, out_ref):
    out_ref[...] = jnp.broadcast_to(jnp.sum(in_ref[...], axis=0, keepdims=True), out_ref.shape)


def leading(grams):
    diag, cross_re, cross_im = grams[:NB], grams[NB : 2 * NB], grams[2 * NB :]
    place = {p: q for q, p in enumerate(PAIRS)}

    def apply(xr, xi):
        ur, ui = [], []
        for a in range(NB):
            r, i = diag[a] * xr[a], diag[a] * xi[a]
            for c in range(NB):
                if c == a:
                    continue
                g = cross_re[place[min(a, c), max(a, c)]]
                h = cross_im[place[min(a, c), max(a, c)]]
                if a < c:
                    r, i = r + (g * xr[c] - h * xi[c]), i + (g * xi[c] + h * xr[c])
                else:
                    r, i = r + (g * xr[c] + h * xi[c]), i + (g * xi[c] - h * xr[c])
            ur.append(r)
            ui.append(i)
        return ur, ui

    xr = [jnp.ones_like(diag[0])] * NB
    xi = [jnp.zeros_like(diag[0])] * NB
    for _ in range(ITERS):
        ur, ui = apply(xr, xi)
        size = sum(r * r + i * i for r, i in zip(ur, ui))
        inverse = lax.rsqrt(size)
        xr, xi = [r * inverse for r in ur], [i * inverse for i in ui]
    ur, ui = apply(xr, xi)
    return xr, xi, sum(a * b + c * d for a, b, c, d in zip(xr, ur, xi, ui))


def modes_kernel(count, in_ref, tab_ref, high_ref, low_ref, modes_ref, energy_ref):
    n_var, n_time, n_pts = high_ref.shape
    total = jnp.sum(in_ref[...], axis=0) * (1.0 / count)
    xr, xi, energy = leading([total[:, KF * q : KF * (q + 1)] for q in range(QS)])
    energy_ref[...] = energy
    factor = lax.rsqrt(jnp.maximum(energy, 0.25))
    cr = [column(x * factor, KF) for x in xr]
    ci = [column(x * factor, KF) for x in xi]
    m_re = m_im = None
    for b in range(NB):
        t_re, t_im = tab_ref[2 * b], tab_ref[2 * b + 1]
        re = cr[b] * t_re - ci[b] * t_im
        im = cr[b] * t_im + ci[b] * t_re
        m_re = re if m_re is None else m_re + re
        m_im = im if m_im is None else m_im + im
    m_high, m_low = halves(jnp.concatenate([m_re, m_im], axis=0))
    tiles = n_pts // LANES
    stride = 2 * n_var * tiles
    for v in range(n_var):
        out = product(m_high, m_low, high_ref[v], low_ref[v])
        for t in range(tiles):
            for c in range(2):
                modes_ref[pl.ds(2 * (v * tiles + t) + c, KF, stride), :] = out[
                    KF * c : KF * (c + 1), LANES * t : LANES * (t + 1)
                ]


def spectra(starts, bins, weights, x, peers):
    n_var, n_time, n_pts = x.shape
    vmem, smem = pltpu.VMEM, pltpu.SMEM
    spec = pl.BlockSpec
    return pl.pallas_call(
        spectra_kernel,
        in_specs=[
            spec(memory_space=smem), spec(memory_space=vmem), spec(memory_space=vmem),
            spec(memory_space=pl.ANY),
        ],
        out_specs=[spec(memory_space=vmem)] * 4,
        out_shape=[
            jax.ShapeDtypeStruct((peers, 1, QS * KF), jnp.float32),
            jax.ShapeDtypeStruct(x.shape, jnp.bfloat16),
            jax.ShapeDtypeStruct(x.shape, jnp.bfloat16),
            jax.ShapeDtypeStruct((2 * NB, KF, n_time), jnp.float32),
        ],
        scratch_shapes=[
            vmem(x.shape, jnp.float32),
            vmem((n_var, 2 * NB * KF, n_pts), jnp.float32),
            vmem((QS * KF, LANES), jnp.float32),
            pltpu.SemaphoreType.DMA((n_var,)),
        ],
        name="spectra",
    )(starts, bins, weights, x)


def body(snapshots, weights, starts, bins):
    n_time, n_var, n_pts = snapshots.shape
    tiles = n_pts // LANES
    n_freq = lax.axis_size(FREQ)
    per_dev = bins.shape[0] // n_freq
    count = float(n_pts * n_freq * lax.axis_size(PTS) * n_var)
    first, second = lax.axis_size(FIRST), lax.axis_size(SECOND)
    gram, high, low, tab = spectra(
        starts, bins[None], weights[None], jnp.transpose(snapshots, (1, 0, 2)), first
    )
    gram = lax.all_to_all(gram, FIRST, 0, 0, tiled=True)
    gram = pl.pallas_call(
        relay_kernel,
        out_shape=jax.ShapeDtypeStruct((second, 1, QS * KF), jnp.float32),
        name="relay",
    )(gram)
    gram = lax.all_to_all(gram, SECOND, 0, 0, tiled=True)
    rows = 2 * n_var * tiles
    vmem = pltpu.VMEM
    modes, energy_all = pl.pallas_call(
        lambda *refs: modes_kernel(count, *refs),
        in_specs=[pl.BlockSpec(memory_space=vmem)] * 4,
        out_specs=[pl.BlockSpec(memory_space=vmem)] * 2,
        out_shape=[
            jax.ShapeDtypeStruct((KF * rows, LANES), jnp.float32),
            jax.ShapeDtypeStruct((1, KF), jnp.float32),
        ],
        name="modes",
    )(gram, tab, high, low)
    modes = modes.reshape(n_freq, per_dev * rows, LANES)
    modes = lax.all_to_all(modes, FREQ, 0, 0, tiled=True)
    modes = modes.reshape(n_freq, per_dev, n_var, tiles, 2, LANES)
    modes = jnp.transpose(modes, (1, 4, 2, 0, 3, 5))
    modes = modes.reshape(per_dev, 2, n_var, n_freq * n_pts)
    energy = lax.dynamic_slice_in_dim(energy_all[0], lax.axis_index(FREQ) * per_dev, per_dev, 0)
    return (modes, energy)


def solution(mesh):
    split = Mesh(mesh.devices.reshape(4, 8, 4, 2), ("freq_0", "freq_1", "pts_0", "pts_1"))
    placed = (P(None, None, PTS_FREQ), P(PTS_FREQ), P(), P())
    return jax.shard_map(
        body,
        mesh=split,
        in_specs=placed,
        out_specs=(P(FREQ, None, None, PTS), P(FREQ)),
        check_vma=False,
    )
```

```python
import functools
import math

import jax
import jax.numpy as jnp
from jax import lax
from jax.experimental import pallas as pl
from jax.experimental.pallas import tpu as pltpu
from jax.sharding import Mesh
from jax.sharding import PartitionSpec as P

NFFT = 128
NB = 3
ITERS = 8
KF = 64
LANES = 128
QS = 9
PAIRS = ((0, 1), (0, 2), (1, 2))
FREQ = ("freq_0", "freq_1")
PTS = ("pts_0", "pts_1")
PTS_FREQ = ("pts_0", "pts_1", "freq_0", "freq_1")
FIRST = ("freq_0", "pts_0")
SECOND = ("freq_1", "pts_1")


def halves(value):
    high = value.astype(jnp.bfloat16)
    return high, (value - high.astype(jnp.float32)).astype(jnp.bfloat16)


def product(a_high, a_low, b_high, b_low):
    def dot(a, b):
        return jnp.dot(a, b, preferred_element_type=jnp.float32)

    return dot(a_high, b_high) + dot(a_high, b_low) + dot(a_low, b_high)


def column(row, n):
    rows = lax.broadcasted_iota(jnp.int32, (n, n), 0)
    cols = lax.broadcasted_iota(jnp.int32, (n, n), 1)
    wide = jnp.broadcast_to(row, (n, n))
    return jnp.sum(jnp.where(rows == cols, wide, jnp.zeros_like(wide)), axis=1, keepdims=True)


def series(square, terms):
    total = jnp.full_like(square, terms[-1])
    for term in terms[-2::-1]:
        total = total * square + term
    return total


def circle(turns):
    quarter = NFFT // 4
    shifted = turns + quarter // 2
    small = (shifted & (quarter - 1)) - quarter // 2
    side = (shifted >> int(math.log2(quarter))) & 3
    angle = small.astype(jnp.float32) * (2.0 * math.pi / NFFT)
    square = angle * angle
    cos = series(square, [(-1.0) ** n / math.factorial(2 * n) for n in range(6)])
    sin = angle * series(square, [(-1.0) ** n / math.factorial(2 * n + 1) for n in range(6)])
    swap = (side & 1) == 1
    first, second = jnp.where(swap, sin, cos), jnp.where(swap, cos, sin)
    return (
        jnp.where((side == 1) | (side == 2), -first, first),
        jnp.where(side >= 2, -second, second),
    )


def tables(starts_ref, bins, tab_ref):
    step = lax.broadcasted_iota(jnp.int32, (KF, NFFT), 1)
    angle = 2.0 * math.pi / NFFT
    scale = 1.0 / math.sqrt(sum((0.5 - 0.5 * math.cos(angle * t)) ** 2 for t in range(NFFT)))
    window = ((0.5 - 0.5 * circle(step[:8])[0]) * scale)[:1]
    slot_bins = column(bins.astype(jnp.float32), KF).astype(jnp.int32)
    cos, sin = circle(slot_bins * step)
    parts = (cos * window, -sin * window)
    zero = jnp.zeros((KF, NFFT), jnp.float32)
    for b in range(NB):
        start = starts_ref[b]
        for c in range(2):
            turned = pltpu.roll(parts[c], start & (NFFT - 1), 1)
            tab_ref[2 * b + c, :, :NFFT] = jnp.where(step >= start, turned, zero)
            tab_ref[2 * b + c, :, NFFT:] = jnp.where(step < start, turned, zero)


def spectra_kernel(
    starts_hbm, bins_hbm, wts_hbm, x_hbm, gram_ref, high_ref, low_ref, tab_ref, x_ref, starts_ref,
    bins_ref, wts_ref, spec_ref, prod_ref, sems,
):
    n_var, n_time, n_pts = x_ref.shape
    moves = [(starts_hbm, starts_ref), (bins_hbm, bins_ref)]
    moves += [(x_hbm.at[v], x_ref.at[v]) for v in range(n_var)] + [(wts_hbm, wts_ref)]
    copies = [pltpu.make_async_copy(a, b, sems.at[i]) for i, (a, b) in enumerate(moves)]
    for copy in copies:
        copy.start()
    copies[0].wait()
    copies[1].wait()
    tables(starts_ref, bins_ref[...], tab_ref)
    t_high, t_low = halves(tab_ref[...].reshape(2 * NB * KF, n_time))
    for copy in copies[2:]:
        copy.wait()
    for v in range(n_var):
        x = x_ref[v]
        high, low = halves(x - jnp.sum(x, axis=0, keepdims=True) * (1.0 / n_time))
        high_ref[v] = high
        low_ref[v] = low
        spec_ref[v] = product(t_high, t_low, high, low)

    def rows(tile, carry):
        first = pl.multiple_of(tile * 8, 8)
        totals = [None] * QS
        for lane in range(0, n_pts, LANES):
            sums = [None] * QS

            def put(q, value):
                sums[q] = value if sums[q] is None else sums[q] + value

            for v in range(n_var):
                s = [
                    spec_ref[v, pl.ds(KF * r + first, 8), lane : lane + LANES]
                    for r in range(2 * NB)
                ]
                re, im = s[0::2], s[1::2]
                for a in range(NB):
                    put(a, re[a] * re[a] + im[a] * im[a])
                for q, (a, c) in enumerate(PAIRS):
                    put(NB + q, re[a] * re[c] + im[a] * im[c])
                    put(2 * NB + q, re[a] * im[c] - im[a] * re[c])
            w = wts_ref[:, lane : lane + LANES]
            for q in range(QS):
                part = sums[q] * w
                totals[q] = part if totals[q] is None else totals[q] + part
        for q in range(QS):
            prod_ref[pl.ds(KF * q + first, 8), :] = totals[q]
        return carry

    lax.fori_loop(0, KF // 8, rows, 0)
    ones = jnp.ones((16, LANES), jnp.bfloat16)
    sums = sum(
        lax.dot_general(ones, p, (((1,), (1,)), ((), ())), preferred_element_type=jnp.float32)
        for p in halves(prod_ref[...])
    )
    gram_ref[...] = jnp.broadcast_to(sums[0:1][None], gram_ref.shape)


def relay_kernel(in_ref, out_ref):
    out_ref[...] = jnp.broadcast_to(jnp.sum(in_ref[...], axis=0, keepdims=True), out_ref.shape)


def leading(grams):
    diag, cross_re, cross_im = grams[:NB], grams[NB : 2 * NB], grams[2 * NB :]
    place = {p: q for q, p in enumerate(PAIRS)}

    def apply(xr, xi):
        ur, ui = [], []
        for a in range(NB):
            r, i = diag[a] * xr[a], diag[a] * xi[a]
            for c in range(NB):
                if c == a:
                    continue
                g = cross_re[place[min(a, c), max(a, c)]]
                h = cross_im[place[min(a, c), max(a, c)]]
                if a < c:
                    r, i = r + (g * xr[c] - h * xi[c]), i + (g * xi[c] + h * xr[c])
                else:
                    r, i = r + (g * xr[c] + h * xi[c]), i + (g * xi[c] - h * xr[c])
            ur.append(r)
            ui.append(i)
        return ur, ui

    xr = [jnp.ones_like(diag[0])] * NB
    xi = [jnp.zeros_like(diag[0])] * NB
    for _ in range(ITERS):
        ur, ui = apply(xr, xi)
        size = sum(r * r + i * i for r, i in zip(ur, ui))
        inverse = lax.rsqrt(size)
        xr, xi = [r * inverse for r in ur], [i * inverse for i in ui]
    ur, ui = apply(xr, xi)
    return xr, xi, sum(a * b + c * d for a, b, c, d in zip(xr, ur, xi, ui))


def modes_kernel(count, in_ref, tab_ref, high_ref, low_ref, modes_ref, energy_ref):
    n_var, n_time, n_pts = high_ref.shape
    total = jnp.sum(in_ref[...], axis=0) * (1.0 / count)
    wide = []
    for first in range(0, QS * KF, LANES):
        part = total[:, first : first + LANES]
        if part.shape[1] == LANES:
            wide += [part, pltpu.roll(part, KF, 1)]
        else:
            wide.append(jnp.concatenate([part, part], axis=1))
    xr, xi, energy = leading(wide)
    per_dev = energy_ref.shape[1]
    shift = lax.rem(LANES - lax.axis_index(FREQ) * per_dev, LANES)
    energy_ref[...] = pltpu.roll(energy, shift, 1)[:, :per_dev]
    factor = lax.rsqrt(jnp.maximum(energy, 0.25))
    zero = jnp.zeros_like(factor)
    turned = jnp.transpose(
        jnp.concatenate([x * factor for x in xr + xi] + [zero, zero], axis=0)
    )
    cr = [turned[:KF, b : b + 1] for b in range(NB)]
    ci = [turned[:KF, NB + b : NB + b + 1] for b in range(NB)]
    m_re = m_im = None
    for b in range(NB):
        t_re, t_im = tab_ref[2 * b], tab_ref[2 * b + 1]
        re = cr[b] * t_re - ci[b] * t_im
        im = cr[b] * t_im + ci[b] * t_re
        m_re = re if m_re is None else m_re + re
        m_im = im if m_im is None else m_im + im
    m_high, m_low = halves(jnp.concatenate([m_re, m_im], axis=0))
    tiles = n_pts // LANES
    stride = 2 * n_var * tiles
    for v in range(n_var):
        out = product(m_high, m_low, high_ref[v], low_ref[v])
        for t in range(tiles):
            for c in range(2):
                modes_ref[pl.ds(2 * (v * tiles + t) + c, KF, stride), :] = out[
                    KF * c : KF * (c + 1), LANES * t : LANES * (t + 1)
                ]


def assemble_kernel(in_ref, out_hbm, sems):
    copies = [
        pltpu.make_async_copy(in_ref.at[:, g], out_hbm.at[g], sems.at[g])
        for g in range(out_hbm.shape[0])
    ]
    for copy in copies:
        copy.start()
    for copy in copies:
        copy.wait()


def spectra(starts, bins, weights, x, peers):
    n_var, n_time, n_pts = x.shape
    vmem, smem = pltpu.VMEM, pltpu.SMEM
    spec = pl.BlockSpec
    return pl.pallas_call(
        spectra_kernel,
        in_specs=[spec(memory_space=pl.ANY)] * 4,
        out_specs=[spec(memory_space=vmem)] * 4,
        out_shape=[
            vmem((peers, 1, QS * KF), jnp.float32),
            vmem(x.shape, jnp.bfloat16),
            vmem(x.shape, jnp.bfloat16),
            vmem((2 * NB, KF, n_time), jnp.float32),
        ],
        scratch_shapes=[
            vmem(x.shape, jnp.float32),
            smem(starts.shape, jnp.int32),
            vmem(bins.shape, jnp.int32),
            vmem(weights.shape, jnp.float32),
            vmem((n_var, 2 * NB * KF, n_pts), jnp.float32),
            vmem((QS * KF, LANES), jnp.float32),
            pltpu.SemaphoreType.DMA((n_var + 3,)),
        ],
        name="spectra",
    )(starts, bins, weights, x)


def body(snapshots, weights, starts, bins):
    n_time, n_var, n_pts = snapshots.shape
    tiles = n_pts // LANES
    n_freq = lax.axis_size(FREQ)
    per_dev = bins.shape[0] // n_freq
    count = float(n_pts * n_freq * lax.axis_size(PTS) * n_var)
    first, second = lax.axis_size(FIRST), lax.axis_size(SECOND)
    gram, high, low, tab = spectra(
        starts, bins[None], weights[None], jnp.transpose(snapshots, (1, 0, 2)), first
    )
    vmem = pltpu.VMEM
    keep = functools.partial(pltpu.with_memory_space_constraint, memory_space=vmem)
    in_vmem = pl.BlockSpec(memory_space=vmem)
    gram = lax.all_to_all(gram, FIRST, 0, 0, tiled=True)
    gram = pl.pallas_call(
        relay_kernel,
        in_specs=[in_vmem],
        out_specs=in_vmem,
        out_shape=vmem((second, 1, QS * KF), jnp.float32),
        name="relay",
    )(keep(gram))
    gram = lax.all_to_all(gram, SECOND, 0, 0, tiled=True)
    rows = 2 * n_var * tiles
    modes, energy = pl.pallas_call(
        functools.partial(modes_kernel, count),
        in_specs=[in_vmem] * 4,
        out_specs=[in_vmem] * 2,
        out_shape=[vmem((KF * rows, LANES), jnp.float32), jax.ShapeDtypeStruct((1, per_dev), jnp.float32)],
        name="modes",
    )(keep(gram), keep(tab), keep(high), keep(low))
    groups = per_dev * n_var
    modes = modes.reshape(n_freq, groups, 2 * tiles, LANES)
    modes = lax.all_to_all(modes, FREQ, 0, 0, tiled=True)
    modes = pl.pallas_call(
        assemble_kernel,
        in_specs=[in_vmem],
        out_specs=pl.BlockSpec(memory_space=pl.ANY),
        out_shape=jax.ShapeDtypeStruct((groups, n_freq, 2 * tiles, LANES), jnp.float32),
        scratch_shapes=[pltpu.SemaphoreType.DMA((groups,))],
        name="assemble",
    )(keep(modes))
    modes = modes.reshape(per_dev, n_var, n_freq * tiles, 2, LANES)
    modes = jnp.transpose(modes, (0, 3, 1, 2, 4)).reshape(per_dev, 2, n_var, n_freq * n_pts)
    return (modes, energy[0])


def solution(mesh):
    split = Mesh(mesh.devices.reshape(4, 8, 4, 2), ("freq_0", "freq_1", "pts_0", "pts_1"))
    placed = (P(None, None, PTS_FREQ), P(PTS_FREQ), P(), P())
    return jax.shard_map(
        body,
        mesh=split,
        in_specs=placed,
        out_specs=(P(FREQ, None, None, PTS), P(FREQ)),
        check_vma=False,
    )
```

```python
import functools
import math

import jax
import jax.numpy as jnp
from jax import lax
from jax.experimental import pallas as pl
from jax.experimental.pallas import tpu as pltpu
from jax.sharding import Mesh
from jax.sharding import PartitionSpec as P

NFFT = 128
NB = 3
ITERS = 8
KF = 64
LANES = 128
QS = 9
PAIRS = ((0, 1), (0, 2), (1, 2))
FREQ = ("freq_0", "freq_1")
PTS = ("pts_0", "pts_1")
PTS_FREQ = ("pts_0", "pts_1", "freq_0", "freq_1")
FIRST = ("freq_0", "pts_0")
SECOND = ("freq_1",)


def halves(value):
    high = value.astype(jnp.bfloat16)
    return high, (value - high.astype(jnp.float32)).astype(jnp.bfloat16)


def product(a_high, a_low, b_high, b_low):
    def dot(a, b):
        return jnp.dot(a, b, preferred_element_type=jnp.float32)

    return dot(a_high, b_high) + dot(a_high, b_low) + dot(a_low, b_high)


def column(row, n):
    rows = lax.broadcasted_iota(jnp.int32, (n, n), 0)
    cols = lax.broadcasted_iota(jnp.int32, (n, n), 1)
    wide = jnp.broadcast_to(row, (n, n))
    return jnp.sum(jnp.where(rows == cols, wide, jnp.zeros_like(wide)), axis=1, keepdims=True)


def series(square, terms):
    total = jnp.full_like(square, terms[-1])
    for term in terms[-2::-1]:
        total = total * square + term
    return total


def circle(turns):
    quarter = NFFT // 4
    shifted = turns + quarter // 2
    small = (shifted & (quarter - 1)) - quarter // 2
    side = (shifted >> int(math.log2(quarter))) & 3
    angle = small.astype(jnp.float32) * (2.0 * math.pi / NFFT)
    square = angle * angle
    cos = series(square, [(-1.0) ** n / math.factorial(2 * n) for n in range(6)])
    sin = angle * series(square, [(-1.0) ** n / math.factorial(2 * n + 1) for n in range(6)])
    swap = (side & 1) == 1
    first, second = jnp.where(swap, sin, cos), jnp.where(swap, cos, sin)
    return (
        jnp.where((side == 1) | (side == 2), -first, first),
        jnp.where(side >= 2, -second, second),
    )


def tables(starts_ref, bins, tab_ref):
    step = lax.broadcasted_iota(jnp.int32, (KF, NFFT), 1)
    angle = 2.0 * math.pi / NFFT
    scale = 1.0 / math.sqrt(sum((0.5 - 0.5 * math.cos(angle * t)) ** 2 for t in range(NFFT)))
    window = ((0.5 - 0.5 * circle(step[:8])[0]) * scale)[:1]
    slot_bins = column(bins.astype(jnp.float32), KF).astype(jnp.int32)
    cos, sin = circle(slot_bins * step)
    parts = (cos * window, -sin * window)
    zero = jnp.zeros((KF, NFFT), jnp.float32)
    for b in range(NB):
        start = starts_ref[b]
        for c in range(2):
            turned = pltpu.roll(parts[c], start & (NFFT - 1), 1)
            tab_ref[2 * b + c, :, :NFFT] = jnp.where(step >= start, turned, zero)
            tab_ref[2 * b + c, :, NFFT:] = jnp.where(step < start, turned, zero)


def spectra_kernel(
    starts_hbm, bins_hbm, wts_hbm, x_hbm, gram_ref, high_ref, low_ref, tab_ref, x_ref, starts_ref,
    bins_ref, wts_ref, spec_ref, sum_ref, sems,
):
    n_var, n_time, n_pts = x_ref.shape
    moves = [(starts_hbm, starts_ref), (bins_hbm, bins_ref)]
    moves += [(x_hbm.at[v], x_ref.at[v]) for v in range(n_var)] + [(wts_hbm, wts_ref)]
    copies = [pltpu.make_async_copy(a, b, sems.at[i]) for i, (a, b) in enumerate(moves)]
    for copy in copies:
        copy.start()
    copies[0].wait()
    copies[1].wait()
    tables(starts_ref, bins_ref[...], tab_ref)
    t_high, t_low = halves(tab_ref[...].reshape(2 * NB * KF, n_time))
    for copy in copies[2:]:
        copy.wait()
    for v in range(n_var):
        x = x_ref[v]
        high, low = halves(x - jnp.sum(x, axis=0, keepdims=True) * (1.0 / n_time))
        high_ref[v] = high
        low_ref[v] = low
        spec_ref[v] = product(t_high, t_low, high, low)
        for first in range(0, KF, 8):
            for lane in range(0, n_pts, LANES):
                s = [
                    spec_ref[v, KF * r + first : KF * r + first + 8, lane : lane + LANES]
                    for r in range(2 * NB)
                ]
                re, im = s[0::2], s[1::2]
                parts = [re[a] * re[a] + im[a] * im[a] for a in range(NB)]
                parts += [re[a] * re[c] + im[a] * im[c] for a, c in PAIRS]
                parts += [re[a] * im[c] - im[a] * re[c] for a, c in PAIRS]
                for q in range(QS):
                    if v > 0:
                        parts[q] = parts[q] + sum_ref[q, first : first + 8, lane : lane + LANES]
                    sum_ref[q, first : first + 8, lane : lane + LANES] = parts[q]
    weighted = sum_ref[...] * wts_ref[...][None]
    prod = sum(weighted[:, :, lane : lane + LANES] for lane in range(0, n_pts, LANES))
    prod = prod.reshape(QS * KF, LANES)
    ones = jnp.ones((16, LANES), jnp.bfloat16)
    sums = sum(
        lax.dot_general(ones, p, (((1,), (1,)), ((), ())), preferred_element_type=jnp.float32)
        for p in halves(prod)
    )
    gram_ref[...] = jnp.broadcast_to(sums[0:1][None], gram_ref.shape)


def relay_kernel(in_ref, out_ref):
    out_ref[...] = jnp.broadcast_to(jnp.sum(in_ref[...], axis=0, keepdims=True), out_ref.shape)


def pair_kernel(one_ref, two_ref, out_ref):
    out_ref[...] = jnp.broadcast_to(one_ref[...] + two_ref[...], out_ref.shape)


def leading(grams):
    diag, cross_re, cross_im = grams[:NB], grams[NB : 2 * NB], grams[2 * NB :]
    place = {p: q for q, p in enumerate(PAIRS)}

    def apply(xr, xi):
        ur, ui = [], []
        for a in range(NB):
            r, i = diag[a] * xr[a], diag[a] * xi[a]
            for c in range(NB):
                if c == a:
                    continue
                g = cross_re[place[min(a, c), max(a, c)]]
                h = cross_im[place[min(a, c), max(a, c)]]
                if a < c:
                    r, i = r + (g * xr[c] - h * xi[c]), i + (g * xi[c] + h * xr[c])
                else:
                    r, i = r + (g * xr[c] + h * xi[c]), i + (g * xi[c] - h * xr[c])
            ur.append(r)
            ui.append(i)
        return ur, ui

    xr = [jnp.ones_like(diag[0])] * NB
    xi = [jnp.zeros_like(diag[0])] * NB
    for _ in range(ITERS):
        ur, ui = apply(xr, xi)
        size = sum(r * r + i * i for r, i in zip(ur, ui))
        inverse = lax.rsqrt(size)
        xr, xi = [r * inverse for r in ur], [i * inverse for i in ui]
    ur, ui = apply(xr, xi)
    return xr, xi, sum(a * b + c * d for a, b, c, d in zip(xr, ur, xi, ui))


def modes_kernel(count, in_ref, tab_ref, high_ref, low_ref, modes_ref, energy_ref):
    n_var, n_time, n_pts = high_ref.shape
    total = jnp.sum(in_ref[...], axis=0) * (1.0 / count)
    wide = []
    for first in range(0, QS * KF, LANES):
        part = total[:, first : first + LANES]
        if part.shape[1] == LANES:
            wide += [part, pltpu.roll(part, KF, 1)]
        else:
            wide.append(jnp.concatenate([part, part], axis=1))
    xr, xi, energy = leading(wide)
    per_dev = energy_ref.shape[1]
    shift = lax.rem(LANES - lax.axis_index(FREQ) * per_dev, LANES)
    energy_ref[...] = pltpu.roll(energy, shift, 1)[:, :per_dev]
    factor = lax.rsqrt(jnp.maximum(energy, 0.25))
    zero = jnp.zeros_like(factor)
    turned = jnp.transpose(
        jnp.concatenate([x * factor for x in xr + xi] + [zero, zero], axis=0)
    )
    cr = [turned[:KF, b : b + 1] for b in range(NB)]
    ci = [turned[:KF, NB + b : NB + b + 1] for b in range(NB)]
    m_re = m_im = None
    for b in range(NB):
        t_re, t_im = tab_ref[2 * b], tab_ref[2 * b + 1]
        re = cr[b] * t_re - ci[b] * t_im
        im = cr[b] * t_im + ci[b] * t_re
        m_re = re if m_re is None else m_re + re
        m_im = im if m_im is None else m_im + im
    m_high, m_low = halves(jnp.concatenate([m_re, m_im], axis=0))
    tiles = n_pts // LANES
    stride = 2 * n_var * tiles
    for v in range(n_var):
        out = product(m_high, m_low, high_ref[v], low_ref[v])
        for t in range(tiles):
            for c in range(2):
                modes_ref[pl.ds(2 * (v * tiles + t) + c, KF, stride), :] = out[
                    KF * c : KF * (c + 1), LANES * t : LANES * (t + 1)
                ]


def assemble_kernel(in_ref, out_hbm, sems):
    copies = [
        pltpu.make_async_copy(in_ref.at[:, g], out_hbm.at[g], sems.at[g])
        for g in range(out_hbm.shape[0])
    ]
    for copy in copies:
        copy.start()
    for copy in copies:
        copy.wait()


def spectra(starts, bins, weights, x, peers):
    n_var, n_time, n_pts = x.shape
    vmem, smem = pltpu.VMEM, pltpu.SMEM
    spec = pl.BlockSpec
    return pl.pallas_call(
        spectra_kernel,
        in_specs=[spec(memory_space=pl.ANY)] * 4,
        out_specs=[spec(memory_space=vmem)] * 4,
        out_shape=[
            vmem((peers, 1, QS * KF), jnp.float32),
            vmem(x.shape, jnp.bfloat16),
            vmem(x.shape, jnp.bfloat16),
            vmem((2 * NB, KF, n_time), jnp.float32),
        ],
        scratch_shapes=[
            vmem(x.shape, jnp.float32),
            smem(starts.shape, jnp.int32),
            vmem(bins.shape, jnp.int32),
            vmem(weights.shape, jnp.float32),
            vmem((n_var, 2 * NB * KF, n_pts), jnp.float32),
            vmem((QS, KF, n_pts), jnp.float32),
            pltpu.SemaphoreType.DMA((n_var + 3,)),
        ],
        name="spectra",
    )(starts, bins, weights, x)


def body(snapshots, weights, starts, bins):
    n_time, n_var, n_pts = snapshots.shape
    tiles = n_pts // LANES
    n_freq = lax.axis_size(FREQ)
    per_dev = bins.shape[0] // n_freq
    count = float(n_pts * n_freq * lax.axis_size(PTS) * n_var)
    first, second = lax.axis_size(FIRST), lax.axis_size(SECOND)
    gram, high, low, tab = spectra(
        starts, bins[None], weights[None], jnp.transpose(snapshots, (1, 0, 2)), 1
    )
    vmem = pltpu.VMEM
    keep = functools.partial(pltpu.with_memory_space_constraint, memory_space=vmem)
    in_vmem = pl.BlockSpec(memory_space=vmem)
    other = lax.ppermute(gram, "pts_1", [(0, 1), (1, 0)])
    gram = pl.pallas_call(
        pair_kernel,
        in_specs=[in_vmem] * 2,
        out_specs=in_vmem,
        out_shape=vmem((first, 1, QS * KF), jnp.float32),
        name="pair",
    )(keep(gram), keep(other))
    gram = lax.all_to_all(gram, FIRST, 0, 0, tiled=True)
    gram = pl.pallas_call(
        relay_kernel,
        in_specs=[in_vmem],
        out_specs=in_vmem,
        out_shape=vmem((second, 1, QS * KF), jnp.float32),
        name="relay",
    )(keep(gram))
    gram = lax.all_to_all(gram, SECOND, 0, 0, tiled=True)
    rows = 2 * n_var * tiles
    modes, energy = pl.pallas_call(
        functools.partial(modes_kernel, count),
        in_specs=[in_vmem] * 4,
        out_specs=[in_vmem] * 2,
        out_shape=[vmem((KF * rows, LANES), jnp.float32), jax.ShapeDtypeStruct((1, per_dev), jnp.float32)],
        name="modes",
    )(keep(gram), keep(tab), keep(high), keep(low))
    groups = per_dev * n_var
    modes = modes.reshape(n_freq, groups, 2 * tiles, LANES)
    modes = lax.all_to_all(modes, FREQ, 0, 0, tiled=True)
    modes = pl.pallas_call(
        assemble_kernel,
        in_specs=[in_vmem],
        out_specs=pl.BlockSpec(memory_space=pl.ANY),
        out_shape=jax.ShapeDtypeStruct((groups, n_freq, 2 * tiles, LANES), jnp.float32),
        scratch_shapes=[pltpu.SemaphoreType.DMA((groups,))],
        name="assemble",
    )(keep(modes))
    modes = modes.reshape(per_dev, n_var, n_freq * tiles, 2, LANES)
    modes = jnp.transpose(modes, (0, 3, 1, 2, 4)).reshape(per_dev, 2, n_var, n_freq * n_pts)
    return (modes, energy[0])


def solution(mesh):
    split = Mesh(mesh.devices.reshape(4, 8, 4, 2), ("freq_0", "freq_1", "pts_0", "pts_1"))
    placed = (P(None, None, PTS_FREQ), P(PTS_FREQ), P(), P())
    return jax.shard_map(
        body,
        mesh=split,
        in_specs=placed,
        out_specs=(P(FREQ, None, None, PTS), P(FREQ)),
        check_vma=False,
    )
```

```python
import functools
import math

import jax
import jax.numpy as jnp
from jax import lax
from jax.experimental import pallas as pl
from jax.experimental.pallas import tpu as pltpu
from jax.sharding import Mesh
from jax.sharding import PartitionSpec as P

NFFT = 128
NB = 3
ITERS = 8
KF = 64
LANES = 128
QS = 9
PAIRS = ((0, 1), (0, 2), (1, 2))
FREQ = ("freq_0", "freq_1")
PTS = ("pts_0", "pts_1")
PTS_FREQ = ("pts_0", "pts_1", "freq_0", "freq_1")


def halves(value):
    high = value.astype(jnp.bfloat16)
    return high, (value - high.astype(jnp.float32)).astype(jnp.bfloat16)


def product(a_high, a_low, b_high, b_low):
    def dot(a, b):
        return jnp.dot(a, b, preferred_element_type=jnp.float32)

    return dot(a_high, b_high) + dot(a_high, b_low) + dot(a_low, b_high)


def column(row, n):
    rows = lax.broadcasted_iota(jnp.int32, (n, n), 0)
    cols = lax.broadcasted_iota(jnp.int32, (n, n), 1)
    wide = jnp.broadcast_to(row, (n, n))
    return jnp.sum(jnp.where(rows == cols, wide, jnp.zeros_like(wide)), axis=1, keepdims=True)


def series(square, terms):
    total = jnp.full_like(square, terms[-1])
    for term in terms[-2::-1]:
        total = total * square + term
    return total


def circle(turns):
    quarter = NFFT // 4
    shifted = turns + quarter // 2
    small = (shifted & (quarter - 1)) - quarter // 2
    side = (shifted >> int(math.log2(quarter))) & 3
    angle = small.astype(jnp.float32) * (2.0 * math.pi / NFFT)
    square = angle * angle
    cos = series(square, [(-1.0) ** n / math.factorial(2 * n) for n in range(6)])
    sin = angle * series(square, [(-1.0) ** n / math.factorial(2 * n + 1) for n in range(6)])
    swap = (side & 1) == 1
    first, second = jnp.where(swap, sin, cos), jnp.where(swap, cos, sin)
    return (
        jnp.where((side == 1) | (side == 2), -first, first),
        jnp.where(side >= 2, -second, second),
    )


def tables(starts_ref, bins, tab_ref):
    step = lax.broadcasted_iota(jnp.int32, (KF, NFFT), 1)
    angle = 2.0 * math.pi / NFFT
    scale = 1.0 / math.sqrt(sum((0.5 - 0.5 * math.cos(angle * t)) ** 2 for t in range(NFFT)))
    window = ((0.5 - 0.5 * circle(step[:8])[0]) * scale)[:1]
    slot_bins = column(bins.astype(jnp.float32), KF).astype(jnp.int32)
    cos, sin = circle(slot_bins * step)
    parts = (cos * window, -sin * window)
    zero = jnp.zeros((KF, NFFT), jnp.float32)
    for b in range(NB):
        start = starts_ref[b]
        for c in range(2):
            turned = pltpu.roll(parts[c], start & (NFFT - 1), 1)
            tab_ref[2 * b + c, :, :NFFT] = jnp.where(step >= start, turned, zero)
            tab_ref[2 * b + c, :, NFFT:] = jnp.where(step < start, turned, zero)


def spectra_kernel(
    starts_hbm, bins_hbm, wts_hbm, x_hbm, gram_ref, high_ref, low_ref, tab_ref, x_ref, starts_ref,
    bins_ref, wts_ref, spec_ref, sum_ref, sems,
):
    n_var, n_time, n_pts = x_ref.shape
    moves = [(starts_hbm, starts_ref), (bins_hbm, bins_ref)]
    moves += [(x_hbm.at[v], x_ref.at[v]) for v in range(n_var)] + [(wts_hbm, wts_ref)]
    copies = [pltpu.make_async_copy(a, b, sems.at[i]) for i, (a, b) in enumerate(moves)]
    for copy in copies:
        copy.start()
    copies[0].wait()
    copies[1].wait()
    tables(starts_ref, bins_ref[...], tab_ref)
    t_high, t_low = halves(tab_ref[...].reshape(2 * NB * KF, n_time))
    for copy in copies[2:]:
        copy.wait()
    for v in range(n_var):
        x = x_ref[v]
        high, low = halves(x - jnp.sum(x, axis=0, keepdims=True) * (1.0 / n_time))
        high_ref[v] = high
        low_ref[v] = low
        spec_ref[v] = product(t_high, t_low, high, low)
        for first in range(0, KF, 8):
            for lane in range(0, n_pts, LANES):
                s = [
                    spec_ref[v, KF * r + first : KF * r + first + 8, lane : lane + LANES]
                    for r in range(2 * NB)
                ]
                re, im = s[0::2], s[1::2]
                parts = [re[a] * re[a] + im[a] * im[a] for a in range(NB)]
                parts += [re[a] * re[c] + im[a] * im[c] for a, c in PAIRS]
                parts += [re[a] * im[c] - im[a] * re[c] for a, c in PAIRS]
                for q in range(QS):
                    if v > 0:
                        parts[q] = parts[q] + sum_ref[q, first : first + 8, lane : lane + LANES]
                    sum_ref[q, first : first + 8, lane : lane + LANES] = parts[q]
    weighted = sum_ref[...] * wts_ref[...][None]
    prod = sum(weighted[:, :, lane : lane + LANES] for lane in range(0, n_pts, LANES))
    prod = prod.reshape(QS * KF, LANES)
    ones = jnp.ones((16, LANES), jnp.bfloat16)
    sums = sum(
        lax.dot_general(ones, p, (((1,), (1,)), ((), ())), preferred_element_type=jnp.float32)
        for p in halves(prod)
    )
    gram_ref[...] = jnp.broadcast_to(sums[0:1][None], gram_ref.shape)


def leading(grams):
    diag, cross_re, cross_im = grams[:NB], grams[NB : 2 * NB], grams[2 * NB :]
    place = {p: q for q, p in enumerate(PAIRS)}

    def apply(xr, xi):
        ur, ui = [], []
        for a in range(NB):
            r, i = diag[a] * xr[a], diag[a] * xi[a]
            for c in range(NB):
                if c == a:
                    continue
                g = cross_re[place[min(a, c), max(a, c)]]
                h = cross_im[place[min(a, c), max(a, c)]]
                if a < c:
                    r, i = r + (g * xr[c] - h * xi[c]), i + (g * xi[c] + h * xr[c])
                else:
                    r, i = r + (g * xr[c] + h * xi[c]), i + (g * xi[c] - h * xr[c])
            ur.append(r)
            ui.append(i)
        return ur, ui

    xr = [jnp.ones_like(diag[0])] * NB
    xi = [jnp.zeros_like(diag[0])] * NB
    for _ in range(ITERS):
        ur, ui = apply(xr, xi)
        size = sum(r * r + i * i for r, i in zip(ur, ui))
        inverse = lax.rsqrt(size)
        xr, xi = [r * inverse for r in ur], [i * inverse for i in ui]
    ur, ui = apply(xr, xi)
    return xr, xi, sum(a * b + c * d for a, b, c, d in zip(xr, ur, xi, ui))


def add_kernel(one_ref, two_ref, out_ref):
    out_ref[...] = jnp.broadcast_to(one_ref[...] + two_ref[...], out_ref.shape)


def add(one, two, copies):
    in_vmem = pl.BlockSpec(memory_space=pltpu.VMEM)
    keep = functools.partial(pltpu.with_memory_space_constraint, memory_space=pltpu.VMEM)
    return pl.pallas_call(
        add_kernel,
        in_specs=[in_vmem] * 2,
        out_specs=in_vmem,
        out_shape=pltpu.VMEM((copies, *one.shape[1:]), jnp.float32),
        name="add",
    )(keep(one), keep(two))


def modes_kernel(count, in_ref, tab_ref, high_ref, low_ref, modes_ref, energy_ref):
    n_var, n_time, n_pts = high_ref.shape
    total = jnp.sum(in_ref[...], axis=0) * (1.0 / count)
    wide = []
    for first in range(0, QS * KF, LANES):
        part = total[:, first : first + LANES]
        if part.shape[1] == LANES:
            wide += [part, pltpu.roll(part, KF, 1)]
        else:
            wide.append(jnp.concatenate([part, part], axis=1))
    xr, xi, energy = leading(wide)
    per_dev = energy_ref.shape[1]
    shift = lax.rem(LANES - lax.axis_index(FREQ) * per_dev, LANES)
    energy_ref[...] = pltpu.roll(energy, shift, 1)[:, :per_dev]
    factor = lax.rsqrt(jnp.maximum(energy, 0.25))
    zero = jnp.zeros_like(factor)
    turned = jnp.transpose(
        jnp.concatenate([x * factor for x in xr + xi] + [zero, zero], axis=0)
    )
    cr = [turned[:KF, b : b + 1] for b in range(NB)]
    ci = [turned[:KF, NB + b : NB + b + 1] for b in range(NB)]
    m_re = m_im = None
    for b in range(NB):
        t_re, t_im = tab_ref[2 * b], tab_ref[2 * b + 1]
        re = cr[b] * t_re - ci[b] * t_im
        im = cr[b] * t_im + ci[b] * t_re
        m_re = re if m_re is None else m_re + re
        m_im = im if m_im is None else m_im + im
    m_high, m_low = halves(jnp.concatenate([m_re, m_im], axis=0))
    tiles = n_pts // LANES
    stride = 2 * n_var * tiles
    for v in range(n_var):
        out = product(m_high, m_low, high_ref[v], low_ref[v])
        for t in range(tiles):
            for c in range(2):
                modes_ref[pl.ds(2 * (v * tiles + t) + c, KF, stride), :] = out[
                    KF * c : KF * (c + 1), LANES * t : LANES * (t + 1)
                ]


def assemble_kernel(in_ref, energy_ref, out_hbm, energy_hbm, sems):
    groups = out_hbm.shape[0]
    copies = [
        pltpu.make_async_copy(in_ref.at[:, g], out_hbm.at[g], sems.at[g]) for g in range(groups)
    ]
    copies.append(pltpu.make_async_copy(energy_ref, energy_hbm, sems.at[groups]))
    for copy in copies:
        copy.start()
    for copy in copies:
        copy.wait()


def spectra(starts, bins, weights, x, peers):
    n_var, n_time, n_pts = x.shape
    vmem, smem = pltpu.VMEM, pltpu.SMEM
    spec = pl.BlockSpec
    return pl.pallas_call(
        spectra_kernel,
        in_specs=[spec(memory_space=pl.ANY)] * 4,
        out_specs=[spec(memory_space=vmem)] * 4,
        out_shape=[
            vmem((peers, 1, QS * KF), jnp.float32),
            vmem(x.shape, jnp.bfloat16),
            vmem(x.shape, jnp.bfloat16),
            vmem((2 * NB, KF, n_time), jnp.float32),
        ],
        scratch_shapes=[
            vmem(x.shape, jnp.float32),
            smem(starts.shape, jnp.int32),
            vmem(bins.shape, jnp.int32),
            vmem(weights.shape, jnp.float32),
            vmem((n_var, 2 * NB * KF, n_pts), jnp.float32),
            vmem((QS, KF, n_pts), jnp.float32),
            pltpu.SemaphoreType.DMA((n_var + 3,)),
        ],
        name="spectra",
    )(starts, bins, weights, x)


def body(snapshots, weights, starts, bins):
    n_time, n_var, n_pts = snapshots.shape
    tiles = n_pts // LANES
    n_freq = lax.axis_size(FREQ)
    per_dev = bins.shape[0] // n_freq
    count = float(n_pts * n_freq * lax.axis_size(PTS) * n_var)
    gram, high, low, tab = spectra(
        starts, bins[None], weights[None], jnp.transpose(snapshots, (1, 0, 2)), 1
    )
    vmem = pltpu.VMEM
    keep = functools.partial(pltpu.with_memory_space_constraint, memory_space=vmem)
    in_vmem = pl.BlockSpec(memory_space=vmem)
    pairings = (("pts_1", 1), ("pts_0", 1), ("pts_0", 3))
    for step, (axis, flip) in enumerate(pairings, 1):
        other = lax.ppermute(gram, axis, [(i, i ^ flip) for i in range(lax.axis_size(axis))])
        gram = add(gram, other, n_freq if step == len(pairings) else 1)
    gram = lax.all_to_all(gram, FREQ, 0, 0, tiled=True)
    rows = 2 * n_var * tiles
    modes, energy = pl.pallas_call(
        functools.partial(modes_kernel, count),
        in_specs=[in_vmem] * 4,
        out_specs=[in_vmem] * 2,
        out_shape=[vmem((KF * rows, LANES), jnp.float32), vmem((1, per_dev), jnp.float32)],
        name="modes",
    )(keep(gram), keep(tab), keep(high), keep(low))
    groups = per_dev * n_var
    modes = modes.reshape(n_freq, groups, 2 * tiles, LANES)
    modes = lax.all_to_all(modes, FREQ, 0, 0, tiled=True)
    modes, energy = pl.pallas_call(
        assemble_kernel,
        in_specs=[in_vmem] * 2,
        out_specs=[pl.BlockSpec(memory_space=pl.ANY)] * 2,
        out_shape=[
            jax.ShapeDtypeStruct((groups, n_freq, 2 * tiles, LANES), jnp.float32),
            jax.ShapeDtypeStruct((1, per_dev), jnp.float32),
        ],
        scratch_shapes=[pltpu.SemaphoreType.DMA((groups + 1,))],
        name="assemble",
    )(keep(modes), keep(energy))
    modes = modes.reshape(per_dev, n_var, n_freq * tiles, 2, LANES)
    modes = jnp.transpose(modes, (0, 3, 1, 2, 4)).reshape(per_dev, 2, n_var, n_freq * n_pts)
    return (modes, energy[0])


def solution(mesh):
    split = Mesh(mesh.devices.reshape(4, 8, 4, 2), ("freq_0", "freq_1", "pts_0", "pts_1"))
    placed = (P(None, None, PTS_FREQ), P(PTS_FREQ), P(), P())
    return jax.shard_map(
        body,
        mesh=split,
        in_specs=placed,
        out_specs=(P(FREQ, None, None, PTS), P(FREQ)),
        check_vma=False,
    )
```

```python
import functools
import math

import jax
import jax.numpy as jnp
from jax import lax
from jax.experimental import pallas as pl
from jax.experimental.pallas import tpu as pltpu
from jax.sharding import Mesh
from jax.sharding import PartitionSpec as P

NFFT = 128
NB = 3
ITERS = 8
KF = 64
LANES = 128
QS = 9
PAIRS = ((0, 1), (0, 2), (1, 2))
FREQ = ("freq_0", "freq_1")
PTS = ("pts_0", "pts_1")
PTS_FREQ = ("pts_0", "pts_1", "freq_0", "freq_1")


def halves(value):
    high = value.astype(jnp.bfloat16)
    return high, (value - high.astype(jnp.float32)).astype(jnp.bfloat16)


def product(a_high, a_low, b_high, b_low):
    def dot(a, b):
        return jnp.dot(a, b, preferred_element_type=jnp.float32)

    return dot(a_high, b_high) + dot(a_high, b_low) + dot(a_low, b_high)


def thirds(value):
    high, low = halves(value)
    rest = value - high.astype(jnp.float32) - low.astype(jnp.float32)
    return high, low, rest.astype(jnp.bfloat16)


def fine_product(a, b):
    def dot(i, j):
        return jnp.dot(a[i], b[j], preferred_element_type=jnp.float32)

    small = dot(1, 1) + dot(0, 2) + dot(2, 0)
    return dot(0, 0) + dot(0, 1) + dot(1, 0) + small


def column(row, n):
    rows = lax.broadcasted_iota(jnp.int32, (n, n), 0)
    cols = lax.broadcasted_iota(jnp.int32, (n, n), 1)
    wide = jnp.broadcast_to(row, (n, n))
    return jnp.sum(jnp.where(rows == cols, wide, jnp.zeros_like(wide)), axis=1, keepdims=True)


def series(square, terms):
    total = jnp.full_like(square, terms[-1])
    for term in terms[-2::-1]:
        total = total * square + term
    return total


def circle(turns):
    quarter = NFFT // 4
    shifted = turns + quarter // 2
    small = (shifted & (quarter - 1)) - quarter // 2
    side = (shifted >> int(math.log2(quarter))) & 3
    angle = small.astype(jnp.float32) * (2.0 * math.pi / NFFT)
    square = angle * angle
    cos = series(square, [(-1.0) ** n / math.factorial(2 * n) for n in range(6)])
    sin = angle * series(square, [(-1.0) ** n / math.factorial(2 * n + 1) for n in range(6)])
    swap = (side & 1) == 1
    first, second = jnp.where(swap, sin, cos), jnp.where(swap, cos, sin)
    return (
        jnp.where((side == 1) | (side == 2), -first, first),
        jnp.where(side >= 2, -second, second),
    )


def tables(starts_ref, bins, tab_ref):
    step = lax.broadcasted_iota(jnp.int32, (KF, NFFT), 1)
    angle = 2.0 * math.pi / NFFT
    scale = 1.0 / math.sqrt(sum((0.5 - 0.5 * math.cos(angle * t)) ** 2 for t in range(NFFT)))
    window = ((0.5 - 0.5 * circle(step[:8])[0]) * scale)[:1]
    slot_bins = column(bins.astype(jnp.float32), KF).astype(jnp.int32)
    cos, sin = circle(slot_bins * step)
    parts = (cos * window, -sin * window)
    zero = jnp.zeros((KF, NFFT), jnp.float32)
    for b in range(NB):
        start = starts_ref[b]
        for c in range(2):
            turned = pltpu.roll(parts[c], start & (NFFT - 1), 1)
            tab_ref[2 * b + c, :, :NFFT] = jnp.where(step >= start, turned, zero)
            tab_ref[2 * b + c, :, NFFT:] = jnp.where(step < start, turned, zero)


def spectra_kernel(
    starts_hbm, bins_hbm, wts_hbm, x_hbm, gram_ref, left_ref, right_ref, tab_ref, x_ref, starts_ref,
    bins_ref, wts_ref, spec_ref, sum_ref, sems,
):
    n_var, n_time, n_pts = x_ref.shape
    moves = [(starts_hbm, starts_ref), (bins_hbm, bins_ref)]
    moves += [(x_hbm.at[v], x_ref.at[v]) for v in range(n_var)] + [(wts_hbm, wts_ref)]
    copies = [pltpu.make_async_copy(a, b, sems.at[i]) for i, (a, b) in enumerate(moves)]
    for copy in copies:
        copy.start()
    copies[0].wait()
    copies[1].wait()
    tables(starts_ref, bins_ref[...], tab_ref)
    t_high, t_low = halves(tab_ref[...].reshape(2 * NB * KF, n_time))
    for copy in copies[2:]:
        copy.wait()
    for v in range(n_var):
        x = x_ref[v]
        centered = x - jnp.sum(x, axis=0, keepdims=True) * (1.0 / n_time)
        left_ref[v], right_ref[v] = centered[:, : n_pts // 2], centered[:, n_pts // 2 :]
        high, low = halves(centered)
        spec_ref[v] = product(t_high, t_low, high, low)
        for first in range(0, KF, 8):
            for lane in range(0, n_pts, LANES):
                s = [
                    spec_ref[v, KF * r + first : KF * r + first + 8, lane : lane + LANES]
                    for r in range(2 * NB)
                ]
                re, im = s[0::2], s[1::2]
                parts = [re[a] * re[a] + im[a] * im[a] for a in range(NB)]
                parts += [re[a] * re[c] + im[a] * im[c] for a, c in PAIRS]
                parts += [re[a] * im[c] - im[a] * re[c] for a, c in PAIRS]
                for q in range(QS):
                    if v > 0:
                        parts[q] = parts[q] + sum_ref[q, first : first + 8, lane : lane + LANES]
                    sum_ref[q, first : first + 8, lane : lane + LANES] = parts[q]
    weighted = sum_ref[...] * wts_ref[...][None]
    prod = sum(weighted[:, :, lane : lane + LANES] for lane in range(0, n_pts, LANES))
    prod = prod.reshape(QS * KF, LANES)
    ones = jnp.ones((16, LANES), jnp.bfloat16)
    sums = sum(
        lax.dot_general(ones, p, (((1,), (1,)), ((), ())), preferred_element_type=jnp.float32)
        for p in halves(prod)
    )
    gram_ref[...] = jnp.broadcast_to(sums[0:1][None], gram_ref.shape)


def leading(grams):
    diag, cross_re, cross_im = grams[:NB], grams[NB : 2 * NB], grams[2 * NB :]
    place = {p: q for q, p in enumerate(PAIRS)}

    def apply(xr, xi):
        ur, ui = [], []
        for a in range(NB):
            r, i = diag[a] * xr[a], diag[a] * xi[a]
            for c in range(NB):
                if c == a:
                    continue
                g = cross_re[place[min(a, c), max(a, c)]]
                h = cross_im[place[min(a, c), max(a, c)]]
                if a < c:
                    r, i = r + (g * xr[c] - h * xi[c]), i + (g * xi[c] + h * xr[c])
                else:
                    r, i = r + (g * xr[c] + h * xi[c]), i + (g * xi[c] - h * xr[c])
            ur.append(r)
            ui.append(i)
        return ur, ui

    xr = [jnp.ones_like(diag[0])] * NB
    xi = [jnp.zeros_like(diag[0])] * NB
    for _ in range(ITERS):
        ur, ui = apply(xr, xi)
        size = sum(r * r + i * i for r, i in zip(ur, ui))
        inverse = lax.rsqrt(size)
        xr, xi = [r * inverse for r in ur], [i * inverse for i in ui]
    ur, ui = apply(xr, xi)
    return xr, xi, sum(a * b + c * d for a, b, c, d in zip(xr, ur, xi, ui))


def add_kernel(one_ref, two_ref, out_ref):
    out_ref[...] = jnp.broadcast_to(one_ref[...] + two_ref[...], out_ref.shape)


def add(one, two, copies):
    in_vmem = pl.BlockSpec(memory_space=pltpu.VMEM)
    keep = functools.partial(pltpu.with_memory_space_constraint, memory_space=pltpu.VMEM)
    return pl.pallas_call(
        add_kernel,
        in_specs=[in_vmem] * 2,
        out_specs=in_vmem,
        out_shape=pltpu.VMEM((copies, *one.shape[1:]), jnp.float32),
        name="add",
    )(keep(one), keep(two))


def modes_kernel(count, in_ref, tab_ref, left_ref, right_ref, modes_ref, energy_ref):
    n_var, n_time, n_pts = left_ref.shape[0], left_ref.shape[1], 2 * left_ref.shape[2]
    total = jnp.sum(in_ref[...], axis=0) * (1.0 / count)
    wide = []
    for first in range(0, QS * KF, LANES):
        part = total[:, first : first + LANES]
        if part.shape[1] == LANES:
            wide += [part, pltpu.roll(part, KF, 1)]
        else:
            wide.append(jnp.concatenate([part, part], axis=1))
    xr, xi, energy = leading(wide)
    per_dev = energy_ref.shape[1]
    shift = lax.rem(LANES - lax.axis_index(FREQ) * per_dev, LANES)
    energy_ref[...] = pltpu.roll(energy, shift, 1)[:, :per_dev]
    factor = lax.rsqrt(jnp.maximum(energy, 0.25))
    zero = jnp.zeros_like(factor)
    turned = jnp.transpose(
        jnp.concatenate([x * factor for x in xr + xi] + [zero, zero], axis=0)
    )
    cr = [turned[:KF, b : b + 1] for b in range(NB)]
    ci = [turned[:KF, NB + b : NB + b + 1] for b in range(NB)]
    m_re = m_im = None
    for b in range(NB):
        t_re, t_im = tab_ref[2 * b], tab_ref[2 * b + 1]
        re = cr[b] * t_re - ci[b] * t_im
        im = cr[b] * t_im + ci[b] * t_re
        m_re = re if m_re is None else m_re + re
        m_im = im if m_im is None else m_im + im
    m_parts = thirds(jnp.concatenate([m_re, m_im], axis=0))
    tiles = n_pts // LANES
    stride = 2 * n_var * tiles
    for v in range(n_var):
        centered = jnp.concatenate([left_ref[v], right_ref[v]], axis=1)
        out = fine_product(m_parts, thirds(centered))
        for t in range(tiles):
            for c in range(2):
                modes_ref[pl.ds(2 * (v * tiles + t) + c, KF, stride), :] = out[
                    KF * c : KF * (c + 1), LANES * t : LANES * (t + 1)
                ]


def assemble_kernel(in_ref, energy_ref, out_hbm, energy_hbm, sems):
    groups = out_hbm.shape[0]
    copies = [
        pltpu.make_async_copy(in_ref.at[:, g], out_hbm.at[g], sems.at[g]) for g in range(groups)
    ]
    copies.append(pltpu.make_async_copy(energy_ref, energy_hbm, sems.at[groups]))
    for copy in copies:
        copy.start()
    for copy in copies:
        copy.wait()


def spectra(starts, bins, weights, x, peers):
    n_var, n_time, n_pts = x.shape
    vmem, smem = pltpu.VMEM, pltpu.SMEM
    spec = pl.BlockSpec
    return pl.pallas_call(
        spectra_kernel,
        in_specs=[spec(memory_space=pl.ANY)] * 4,
        out_specs=[spec(memory_space=vmem)] * 4,
        out_shape=[
            vmem((peers, 1, QS * KF), jnp.float32),
            vmem((n_var, n_time, n_pts // 2), jnp.float32),
            vmem((n_var, n_time, n_pts // 2), jnp.float32),
            vmem((2 * NB, KF, n_time), jnp.float32),
        ],
        scratch_shapes=[
            vmem(x.shape, jnp.float32),
            smem(starts.shape, jnp.int32),
            vmem(bins.shape, jnp.int32),
            vmem(weights.shape, jnp.float32),
            vmem((n_var, 2 * NB * KF, n_pts), jnp.float32),
            vmem((QS, KF, n_pts), jnp.float32),
            pltpu.SemaphoreType.DMA((n_var + 3,)),
        ],
        name="spectra",
    )(starts, bins, weights, x)


def body(snapshots, weights, starts, bins):
    n_time, n_var, n_pts = snapshots.shape
    tiles = n_pts // LANES
    n_freq = lax.axis_size(FREQ)
    per_dev = bins.shape[0] // n_freq
    count = float(n_pts * n_freq * lax.axis_size(PTS) * n_var)
    gram, left, right, tab = spectra(
        starts, bins[None], weights[None], jnp.transpose(snapshots, (1, 0, 2)), 1
    )
    vmem = pltpu.VMEM
    keep = functools.partial(pltpu.with_memory_space_constraint, memory_space=vmem)
    in_vmem = pl.BlockSpec(memory_space=vmem)
    pairings = (("pts_1", 1), ("pts_0", 1), ("pts_0", 3))
    for step, (axis, flip) in enumerate(pairings, 1):
        other = lax.ppermute(gram, axis, [(i, i ^ flip) for i in range(lax.axis_size(axis))])
        gram = add(gram, other, n_freq if step == len(pairings) else 1)
    gram = lax.all_to_all(gram, FREQ, 0, 0, tiled=True)
    rows = 2 * n_var * tiles
    modes, energy = pl.pallas_call(
        functools.partial(modes_kernel, count),
        in_specs=[in_vmem] * 4,
        out_specs=[in_vmem] * 2,
        out_shape=[vmem((KF * rows, LANES), jnp.float32), vmem((1, per_dev), jnp.float32)],
        name="modes",
    )(keep(gram), keep(tab), keep(left), keep(right))
    groups = per_dev * n_var
    modes = modes.reshape(n_freq, groups, 2 * tiles, LANES)
    modes = lax.all_to_all(modes, FREQ, 0, 0, tiled=True)
    modes, energy = pl.pallas_call(
        assemble_kernel,
        in_specs=[in_vmem] * 2,
        out_specs=[pl.BlockSpec(memory_space=pl.ANY)] * 2,
        out_shape=[
            jax.ShapeDtypeStruct((groups, n_freq, 2 * tiles, LANES), jnp.float32),
            jax.ShapeDtypeStruct((1, per_dev), jnp.float32),
        ],
        scratch_shapes=[pltpu.SemaphoreType.DMA((groups + 1,))],
        name="assemble",
    )(keep(modes), keep(energy))
    modes = modes.reshape(per_dev, n_var, n_freq * tiles, 2, LANES)
    modes = jnp.transpose(modes, (0, 3, 1, 2, 4)).reshape(per_dev, 2, n_var, n_freq * n_pts)
    return (modes, energy[0])


def solution(mesh):
    split = Mesh(mesh.devices.reshape(4, 8, 4, 2), ("freq_0", "freq_1", "pts_0", "pts_1"))
    placed = (P(None, None, PTS_FREQ), P(PTS_FREQ), P(), P())
    return jax.shard_map(
        body,
        mesh=split,
        in_specs=placed,
        out_specs=(P(FREQ, None, None, PTS), P(FREQ)),
        check_vma=False,
    )
```

```python
import functools
import math

import jax
import jax.numpy as jnp
from jax import lax
from jax.experimental import pallas as pl
from jax.experimental.pallas import tpu as pltpu
from jax.sharding import Mesh
from jax.sharding import PartitionSpec as P

NFFT = 128
NB = 3
ITERS = 8
KF = 64
LANES = 128
QS = 9
PAIRS = ((0, 1), (0, 2), (1, 2))
FREQ = ("freq_0", "freq_1")
PTS = ("pts_0", "pts_1")
PTS_FREQ = ("pts_0", "pts_1", "freq_0", "freq_1")


def halves(value):
    high = value.astype(jnp.bfloat16)
    return high, (value - high.astype(jnp.float32)).astype(jnp.bfloat16)


def product(a_high, a_low, b_high, b_low):
    def dot(a, b):
        return jnp.dot(a, b, preferred_element_type=jnp.float32)

    return dot(a_high, b_high) + dot(a_high, b_low) + dot(a_low, b_high)


def thirds(value):
    high, low = halves(value)
    rest = value - high.astype(jnp.float32) - low.astype(jnp.float32)
    return high, low, rest.astype(jnp.bfloat16)


def fine_product(a, b):
    def dot(i, j):
        return jnp.dot(a[i], b[j], preferred_element_type=jnp.float32)

    small = dot(1, 1) + dot(0, 2) + dot(2, 0)
    return dot(0, 0) + dot(0, 1) + dot(1, 0) + small


def column(row, n):
    rows = lax.broadcasted_iota(jnp.int32, (n, n), 0)
    cols = lax.broadcasted_iota(jnp.int32, (n, n), 1)
    wide = jnp.broadcast_to(row, (n, n))
    return jnp.sum(jnp.where(rows == cols, wide, jnp.zeros_like(wide)), axis=1, keepdims=True)


def series(square, terms):
    total = jnp.full_like(square, terms[-1])
    for term in terms[-2::-1]:
        total = total * square + term
    return total


def circle(turns):
    quarter = NFFT // 4
    shifted = turns + quarter // 2
    small = (shifted & (quarter - 1)) - quarter // 2
    side = (shifted >> int(math.log2(quarter))) & 3
    angle = small.astype(jnp.float32) * (2.0 * math.pi / NFFT)
    square = angle * angle
    cos = series(square, [(-1.0) ** n / math.factorial(2 * n) for n in range(6)])
    sin = angle * series(square, [(-1.0) ** n / math.factorial(2 * n + 1) for n in range(6)])
    swap = (side & 1) == 1
    first, second = jnp.where(swap, sin, cos), jnp.where(swap, cos, sin)
    return (
        jnp.where((side == 1) | (side == 2), -first, first),
        jnp.where(side >= 2, -second, second),
    )


def tables(starts_ref, bins, tab_ref):
    step = lax.broadcasted_iota(jnp.int32, (KF, NFFT), 1)
    angle = 2.0 * math.pi / NFFT
    scale = 1.0 / math.sqrt(sum((0.5 - 0.5 * math.cos(angle * t)) ** 2 for t in range(NFFT)))
    window = ((0.5 - 0.5 * circle(step[:8])[0]) * scale)[:1]
    slot_bins = column(bins.astype(jnp.float32), KF).astype(jnp.int32)
    cos, sin = circle(slot_bins * step)
    parts = (cos * window, -sin * window)
    zero = jnp.zeros((KF, NFFT), jnp.float32)
    for b in range(NB):
        start = starts_ref[b]
        for c in range(2):
            turned = pltpu.roll(parts[c], start & (NFFT - 1), 1)
            tab_ref[2 * b + c, :, :NFFT] = jnp.where(step >= start, turned, zero)
            tab_ref[2 * b + c, :, NFFT:] = jnp.where(step < start, turned, zero)


def spectra_kernel(
    starts_hbm, bins_hbm, wts_hbm, x_hbm, gram_ref, left_ref, right_ref, tab_ref, x_ref, starts_ref,
    bins_ref, wts_ref, spec_ref, sum_ref, sems,
):
    n_var, n_time, n_pts = x_ref.shape
    moves = [(starts_hbm, starts_ref), (bins_hbm, bins_ref)]
    moves += [(x_hbm.at[v], x_ref.at[v]) for v in range(n_var)] + [(wts_hbm, wts_ref)]
    copies = [pltpu.make_async_copy(a, b, sems.at[i]) for i, (a, b) in enumerate(moves)]
    for copy in copies:
        copy.start()
    copies[0].wait()
    copies[1].wait()
    tables(starts_ref, bins_ref[...], tab_ref)
    t_high, t_low = halves(tab_ref[...].reshape(2 * NB * KF, n_time))
    for copy in copies[2:]:
        copy.wait()
    for v in range(n_var):
        x = x_ref[v]
        centered = x - jnp.sum(x, axis=0, keepdims=True) * (1.0 / n_time)
        left_ref[v], right_ref[v] = centered[:, : n_pts // 2], centered[:, n_pts // 2 :]
        high, low = halves(centered)
        spec_ref[v] = product(t_high, t_low, high, low)
        for first in range(0, KF, 8):
            for lane in range(0, n_pts, LANES):
                s = [
                    spec_ref[v, KF * r + first : KF * r + first + 8, lane : lane + LANES]
                    for r in range(2 * NB)
                ]
                re, im = s[0::2], s[1::2]
                parts = [re[a] * re[a] + im[a] * im[a] for a in range(NB)]
                parts += [re[a] * re[c] + im[a] * im[c] for a, c in PAIRS]
                parts += [re[a] * im[c] - im[a] * re[c] for a, c in PAIRS]
                for q in range(QS):
                    if v > 0:
                        parts[q] = parts[q] + sum_ref[q, first : first + 8, lane : lane + LANES]
                    sum_ref[q, first : first + 8, lane : lane + LANES] = parts[q]
    weighted = sum_ref[...] * wts_ref[...][None]
    prod = sum(weighted[:, :, lane : lane + LANES] for lane in range(0, n_pts, LANES))
    prod = prod.reshape(QS * KF, LANES)
    ones = jnp.ones((16, LANES), jnp.bfloat16)
    sums = sum(
        lax.dot_general(ones, p, (((1,), (1,)), ((), ())), preferred_element_type=jnp.float32)
        for p in halves(prod)
    )
    gram_ref[...] = jnp.broadcast_to(sums[0:1][None], gram_ref.shape)


def leading(grams):
    diag, cross_re, cross_im = grams[:NB], grams[NB : 2 * NB], grams[2 * NB :]
    place = {p: q for q, p in enumerate(PAIRS)}

    def apply(xr, xi):
        ur, ui = [], []
        for a in range(NB):
            r, i = diag[a] * xr[a], diag[a] * xi[a]
            for c in range(NB):
                if c == a:
                    continue
                g = cross_re[place[min(a, c), max(a, c)]]
                h = cross_im[place[min(a, c), max(a, c)]]
                if a < c:
                    r, i = r + (g * xr[c] - h * xi[c]), i + (g * xi[c] + h * xr[c])
                else:
                    r, i = r + (g * xr[c] + h * xi[c]), i + (g * xi[c] - h * xr[c])
            ur.append(r)
            ui.append(i)
        return ur, ui

    xr = [jnp.ones_like(diag[0])] * NB
    xi = [jnp.zeros_like(diag[0])] * NB
    for _ in range(ITERS):
        ur, ui = apply(xr, xi)
        size = sum(r * r + i * i for r, i in zip(ur, ui))
        inverse = lax.rsqrt(size)
        xr, xi = [r * inverse for r in ur], [i * inverse for i in ui]
    ur, ui = apply(xr, xi)
    return xr, xi, sum(a * b + c * d for a, b, c, d in zip(xr, ur, xi, ui))


def add_kernel(one_ref, two_ref, out_ref):
    out_ref[...] = jnp.broadcast_to(one_ref[...] + two_ref[...], out_ref.shape)


def add(one, two, copies):
    in_vmem = pl.BlockSpec(memory_space=pltpu.VMEM)
    keep = functools.partial(pltpu.with_memory_space_constraint, memory_space=pltpu.VMEM)
    return pl.pallas_call(
        add_kernel,
        in_specs=[in_vmem] * 2,
        out_specs=in_vmem,
        out_shape=pltpu.VMEM((copies, *one.shape[1:]), jnp.float32),
        name="add",
    )(keep(one), keep(two))


def modes_kernel(count, in_ref, tab_ref, left_ref, right_ref, modes_ref, energy_ref, split_ref):
    n_var, n_time, n_pts = left_ref.shape[0], left_ref.shape[1], 2 * left_ref.shape[2]
    for v in range(n_var):
        for i, part in enumerate(thirds(jnp.concatenate([left_ref[v], right_ref[v]], axis=1))):
            split_ref[i, v] = part
    total = jnp.sum(in_ref[...], axis=0) * (1.0 / count)
    wide = []
    for first in range(0, QS * KF, LANES):
        part = total[:, first : first + LANES]
        if part.shape[1] == LANES:
            wide += [part, pltpu.roll(part, KF, 1)]
        else:
            wide.append(jnp.concatenate([part, part], axis=1))
    xr, xi, energy = leading(wide)
    per_dev = energy_ref.shape[1]
    shift = lax.rem(LANES - lax.axis_index(FREQ) * per_dev, LANES)
    energy_ref[...] = pltpu.roll(energy, shift, 1)[:, :per_dev]
    factor = lax.rsqrt(jnp.maximum(energy, 0.25))
    zero = jnp.zeros_like(factor)
    turned = jnp.transpose(
        jnp.concatenate([x * factor for x in xr + xi] + [zero, zero], axis=0)
    )
    cr = [turned[:KF, b : b + 1] for b in range(NB)]
    ci = [turned[:KF, NB + b : NB + b + 1] for b in range(NB)]
    m_re = m_im = None
    for b in range(NB):
        t_re, t_im = tab_ref[2 * b], tab_ref[2 * b + 1]
        re = cr[b] * t_re - ci[b] * t_im
        im = cr[b] * t_im + ci[b] * t_re
        m_re = re if m_re is None else m_re + re
        m_im = im if m_im is None else m_im + im
    m_parts = thirds(jnp.concatenate([m_re, m_im], axis=0))
    tiles = n_pts // LANES
    stride = 2 * n_var * tiles
    for v in range(n_var):
        out = fine_product(m_parts, [split_ref[i, v] for i in range(3)])
        for t in range(tiles):
            for c in range(2):
                modes_ref[pl.ds(2 * (v * tiles + t) + c, KF, stride), :] = out[
                    KF * c : KF * (c + 1), LANES * t : LANES * (t + 1)
                ]


def assemble_kernel(in_ref, energy_ref, out_hbm, energy_hbm, sems):
    groups = out_hbm.shape[0]
    copies = [
        pltpu.make_async_copy(in_ref.at[:, g], out_hbm.at[g], sems.at[g]) for g in range(groups)
    ]
    copies.append(pltpu.make_async_copy(energy_ref, energy_hbm, sems.at[groups]))
    for copy in copies:
        copy.start()
    for copy in copies:
        copy.wait()


def spectra(starts, bins, weights, x, peers):
    n_var, n_time, n_pts = x.shape
    vmem, smem = pltpu.VMEM, pltpu.SMEM
    spec = pl.BlockSpec
    return pl.pallas_call(
        spectra_kernel,
        in_specs=[spec(memory_space=pl.ANY)] * 4,
        out_specs=[spec(memory_space=vmem)] * 4,
        out_shape=[
            vmem((peers, 1, QS * KF), jnp.float32),
            vmem((n_var, n_time, n_pts // 2), jnp.float32),
            vmem((n_var, n_time, n_pts // 2), jnp.float32),
            vmem((2 * NB, KF, n_time), jnp.float32),
        ],
        scratch_shapes=[
            vmem(x.shape, jnp.float32),
            smem(starts.shape, jnp.int32),
            vmem(bins.shape, jnp.int32),
            vmem(weights.shape, jnp.float32),
            vmem((n_var, 2 * NB * KF, n_pts), jnp.float32),
            vmem((QS, KF, n_pts), jnp.float32),
            pltpu.SemaphoreType.DMA((n_var + 3,)),
        ],
        name="spectra",
    )(starts, bins, weights, x)


def body(snapshots, weights, starts, bins):
    n_time, n_var, n_pts = snapshots.shape
    tiles = n_pts // LANES
    n_freq = lax.axis_size(FREQ)
    per_dev = bins.shape[0] // n_freq
    count = float(n_pts * n_freq * lax.axis_size(PTS) * n_var)
    gram, left, right, tab = spectra(
        starts, bins[None], weights[None], jnp.transpose(snapshots, (1, 0, 2)), 1
    )
    vmem = pltpu.VMEM
    keep = functools.partial(pltpu.with_memory_space_constraint, memory_space=vmem)
    in_vmem = pl.BlockSpec(memory_space=vmem)
    pairings = (("pts_1", 1), ("pts_0", 1), ("pts_0", 3))
    for step, (axis, flip) in enumerate(pairings, 1):
        other = lax.ppermute(gram, axis, [(i, i ^ flip) for i in range(lax.axis_size(axis))])
        gram = add(gram, other, n_freq if step == len(pairings) else 1)
    gram = lax.all_to_all(gram, FREQ, 0, 0, tiled=True)
    rows = 2 * n_var * tiles
    modes, energy = pl.pallas_call(
        functools.partial(modes_kernel, count),
        in_specs=[in_vmem] * 4,
        out_specs=[in_vmem] * 2,
        out_shape=[vmem((KF * rows, LANES), jnp.float32), vmem((1, per_dev), jnp.float32)],
        scratch_shapes=[vmem((3, n_var, n_time, n_pts), jnp.bfloat16)],
        name="modes",
    )(keep(gram), keep(tab), keep(left), keep(right))
    groups = per_dev * n_var
    modes = modes.reshape(n_freq, groups, 2 * tiles, LANES)
    modes = lax.all_to_all(modes, FREQ, 0, 0, tiled=True)
    modes, energy = pl.pallas_call(
        assemble_kernel,
        in_specs=[in_vmem] * 2,
        out_specs=[pl.BlockSpec(memory_space=pl.ANY)] * 2,
        out_shape=[
            jax.ShapeDtypeStruct((groups, n_freq, 2 * tiles, LANES), jnp.float32),
            jax.ShapeDtypeStruct((1, per_dev), jnp.float32),
        ],
        scratch_shapes=[pltpu.SemaphoreType.DMA((groups + 1,))],
        name="assemble",
    )(keep(modes), keep(energy))
    modes = modes.reshape(per_dev, n_var, n_freq * tiles, 2, LANES)
    modes = jnp.transpose(modes, (0, 3, 1, 2, 4)).reshape(per_dev, 2, n_var, n_freq * n_pts)
    return (modes, energy[0])


def solution(mesh):
    split = Mesh(mesh.devices.reshape(4, 8, 4, 2), ("freq_0", "freq_1", "pts_0", "pts_1"))
    placed = (P(None, None, PTS_FREQ), P(PTS_FREQ), P(), P())
    return jax.shard_map(
        body,
        mesh=split,
        in_specs=placed,
        out_specs=(P(FREQ, None, None, PTS), P(FREQ)),
        check_vma=False,
    )
```

```python
import functools
import math

import jax
import jax.numpy as jnp
from jax import lax
from jax.experimental import pallas as pl
from jax.experimental.pallas import tpu as pltpu
from jax.sharding import Mesh
from jax.sharding import PartitionSpec as P

NFFT = 128
NB = 3
ITERS = 8
KF = 64
LANES = 128
QS = 9
PAIRS = ((0, 1), (0, 2), (1, 2))
FREQ = ("freq_0", "freq_1")
PTS = ("pts_0", "pts_1")
PTS_FREQ = ("pts_0", "pts_1", "freq_0", "freq_1")


def halves(value):
    high = value.astype(jnp.bfloat16)
    return high, (value - high.astype(jnp.float32)).astype(jnp.bfloat16)


def product(a_high, a_low, b_high, b_low):
    def dot(a, b):
        return jnp.dot(a, b, preferred_element_type=jnp.float32)

    return dot(a_high, b_high) + dot(a_high, b_low) + dot(a_low, b_high)


def thirds(value):
    high, low = halves(value)
    rest = value - high.astype(jnp.float32) - low.astype(jnp.float32)
    return high, low, rest.astype(jnp.bfloat16)


def fine_product(a, b):
    def dot(i, j):
        return jnp.dot(a[i], b[j], preferred_element_type=jnp.float32)

    small = dot(1, 1) + dot(0, 2) + dot(2, 0)
    return dot(0, 0) + dot(0, 1) + dot(1, 0) + small


def column(row, n):
    rows = lax.broadcasted_iota(jnp.int32, (n, n), 0)
    cols = lax.broadcasted_iota(jnp.int32, (n, n), 1)
    wide = jnp.broadcast_to(row, (n, n))
    return jnp.sum(jnp.where(rows == cols, wide, jnp.zeros_like(wide)), axis=1, keepdims=True)


def series(square, terms):
    total = jnp.full_like(square, terms[-1])
    for term in terms[-2::-1]:
        total = total * square + term
    return total


def circle(turns):
    quarter = NFFT // 4
    shifted = turns + quarter // 2
    small = (shifted & (quarter - 1)) - quarter // 2
    side = (shifted >> int(math.log2(quarter))) & 3
    angle = small.astype(jnp.float32) * (2.0 * math.pi / NFFT)
    square = angle * angle
    cos = series(square, [(-1.0) ** n / math.factorial(2 * n) for n in range(6)])
    sin = angle * series(square, [(-1.0) ** n / math.factorial(2 * n + 1) for n in range(6)])
    swap = (side & 1) == 1
    first, second = jnp.where(swap, sin, cos), jnp.where(swap, cos, sin)
    return (
        jnp.where((side == 1) | (side == 2), -first, first),
        jnp.where(side >= 2, -second, second),
    )


def tables(starts_ref, bins, tab_ref):
    step = lax.broadcasted_iota(jnp.int32, (KF, NFFT), 1)
    angle = 2.0 * math.pi / NFFT
    scale = 1.0 / math.sqrt(sum((0.5 - 0.5 * math.cos(angle * t)) ** 2 for t in range(NFFT)))
    window = ((0.5 - 0.5 * circle(step[:8])[0]) * scale)[:1]
    slot_bins = column(bins.astype(jnp.float32), KF).astype(jnp.int32)
    cos, sin = circle(slot_bins * step)
    parts = (cos * window, -sin * window)
    zero = jnp.zeros((KF, NFFT), jnp.float32)
    for b in range(NB):
        start = starts_ref[b]
        for c in range(2):
            turned = pltpu.roll(parts[c], start & (NFFT - 1), 1)
            tab_ref[2 * b + c, :, :NFFT] = jnp.where(step >= start, turned, zero)
            tab_ref[2 * b + c, :, NFFT:] = jnp.where(step < start, turned, zero)


def spectra_kernel(
    starts_hbm, bins_hbm, wts_hbm, x_hbm, gram_ref, left_ref, right_ref, tab_ref, x_ref, starts_ref,
    bins_ref, wts_ref, spec_ref, sum_ref, sems,
):
    n_var, n_time, n_pts = x_ref.shape
    moves = [(starts_hbm, starts_ref), (bins_hbm, bins_ref)]
    moves += [(x_hbm.at[v], x_ref.at[v]) for v in range(n_var)] + [(wts_hbm, wts_ref)]
    copies = [pltpu.make_async_copy(a, b, sems.at[i]) for i, (a, b) in enumerate(moves)]
    for copy in copies:
        copy.start()
    copies[0].wait()
    copies[1].wait()
    tables(starts_ref, bins_ref[...], tab_ref)
    t_high, t_low = halves(tab_ref[...].reshape(2 * NB * KF, n_time))
    for copy in copies[2:]:
        copy.wait()
    for v in range(n_var):
        x = x_ref[v]
        centered = x - jnp.sum(x, axis=0, keepdims=True) * (1.0 / n_time)
        left_ref[v], right_ref[v] = centered[:, : n_pts // 2], centered[:, n_pts // 2 :]
        high, low = halves(centered)
        spec_ref[v] = product(t_high, t_low, high, low)
        if v % 2 == 0 and v < n_var - 1:
            continue
        group = [v] if v % 2 == 0 else [v - 1, v]
        for first in range(0, KF, 8):
            for lane in range(0, n_pts, LANES):
                total = None
                for u in group:
                    s = [
                        spec_ref[u, KF * r + first : KF * r + first + 8, lane : lane + LANES]
                        for r in range(2 * NB)
                    ]
                    re, im = s[0::2], s[1::2]
                    parts = [re[a] * re[a] + im[a] * im[a] for a in range(NB)]
                    parts += [re[a] * re[c] + im[a] * im[c] for a, c in PAIRS]
                    parts += [re[a] * im[c] - im[a] * re[c] for a, c in PAIRS]
                    total = parts if total is None else [p + t for p, t in zip(parts, total)]
                for q in range(QS):
                    if group[0] > 0:
                        total[q] = total[q] + sum_ref[q, first : first + 8, lane : lane + LANES]
                    sum_ref[q, first : first + 8, lane : lane + LANES] = total[q]
    weighted = sum_ref[...] * wts_ref[...][None]
    prod = sum(weighted[:, :, lane : lane + LANES] for lane in range(0, n_pts, LANES))
    prod = prod.reshape(QS * KF, LANES)
    ones = jnp.ones((16, LANES), jnp.bfloat16)
    sums = sum(
        lax.dot_general(ones, p, (((1,), (1,)), ((), ())), preferred_element_type=jnp.float32)
        for p in halves(prod)
    )
    gram_ref[...] = jnp.broadcast_to(sums[0:1][None], gram_ref.shape)


def leading(grams):
    diag, cross_re, cross_im = grams[:NB], grams[NB : 2 * NB], grams[2 * NB :]
    place = {p: q for q, p in enumerate(PAIRS)}

    def apply(xr, xi):
        ur, ui = [], []
        for a in range(NB):
            r, i = diag[a] * xr[a], diag[a] * xi[a]
            for c in range(NB):
                if c == a:
                    continue
                g = cross_re[place[min(a, c), max(a, c)]]
                h = cross_im[place[min(a, c), max(a, c)]]
                if a < c:
                    r, i = r + (g * xr[c] - h * xi[c]), i + (g * xi[c] + h * xr[c])
                else:
                    r, i = r + (g * xr[c] + h * xi[c]), i + (g * xi[c] - h * xr[c])
            ur.append(r)
            ui.append(i)
        return ur, ui

    xr = [jnp.ones_like(diag[0])] * NB
    xi = [jnp.zeros_like(diag[0])] * NB
    for _ in range(ITERS):
        ur, ui = apply(xr, xi)
        size = sum(r * r + i * i for r, i in zip(ur, ui))
        inverse = lax.rsqrt(size)
        xr, xi = [r * inverse for r in ur], [i * inverse for i in ui]
    ur, ui = apply(xr, xi)
    return xr, xi, sum(a * b + c * d for a, b, c, d in zip(xr, ur, xi, ui))


def add_kernel(one_ref, two_ref, out_ref):
    out_ref[...] = jnp.broadcast_to(one_ref[...] + two_ref[...], out_ref.shape)


def add(one, two, copies):
    in_vmem = pl.BlockSpec(memory_space=pltpu.VMEM)
    keep = functools.partial(pltpu.with_memory_space_constraint, memory_space=pltpu.VMEM)
    return pl.pallas_call(
        add_kernel,
        in_specs=[in_vmem] * 2,
        out_specs=in_vmem,
        out_shape=pltpu.VMEM((copies, *one.shape[1:]), jnp.float32),
        name="add",
    )(keep(one), keep(two))


def modes_kernel(count, in_ref, tab_ref, left_ref, right_ref, modes_ref, energy_ref, split_ref):
    n_var, n_time, n_pts = left_ref.shape[0], left_ref.shape[1], 2 * left_ref.shape[2]
    for v in range(n_var):
        for i, part in enumerate(thirds(jnp.concatenate([left_ref[v], right_ref[v]], axis=1))):
            split_ref[i, v] = part
    total = jnp.sum(in_ref[...], axis=0) * (1.0 / count)
    wide = []
    for first in range(0, QS * KF, LANES):
        part = total[:, first : first + LANES]
        if part.shape[1] == LANES:
            wide += [part, pltpu.roll(part, KF, 1)]
        else:
            wide.append(jnp.concatenate([part, part], axis=1))
    xr, xi, energy = leading(wide)
    per_dev = energy_ref.shape[1]
    shift = lax.rem(LANES - lax.axis_index(FREQ) * per_dev, LANES)
    energy_ref[...] = pltpu.roll(energy, shift, 1)[:, :per_dev]
    factor = lax.rsqrt(jnp.maximum(energy, 0.25))
    zero = jnp.zeros_like(factor)
    turned = jnp.transpose(
        jnp.concatenate([x * factor for x in xr + xi] + [zero, zero], axis=0)
    )
    cr = [turned[:KF, b : b + 1] for b in range(NB)]
    ci = [turned[:KF, NB + b : NB + b + 1] for b in range(NB)]
    m_re = m_im = None
    for b in range(NB):
        t_re, t_im = tab_ref[2 * b], tab_ref[2 * b + 1]
        re = cr[b] * t_re - ci[b] * t_im
        im = cr[b] * t_im + ci[b] * t_re
        m_re = re if m_re is None else m_re + re
        m_im = im if m_im is None else m_im + im
    m_parts = thirds(jnp.concatenate([m_re, m_im], axis=0))
    tiles = n_pts // LANES
    stride = 2 * n_var * tiles
    for v in range(n_var):
        out = fine_product(m_parts, [split_ref[i, v] for i in range(3)])
        for t in range(tiles):
            for c in range(2):
                modes_ref[pl.ds(2 * (v * tiles + t) + c, KF, stride), :] = out[
                    KF * c : KF * (c + 1), LANES * t : LANES * (t + 1)
                ]


def assemble_kernel(in_ref, energy_ref, out_hbm, energy_hbm, sems):
    groups = out_hbm.shape[0]
    copies = [
        pltpu.make_async_copy(in_ref.at[:, g], out_hbm.at[g], sems.at[g]) for g in range(groups)
    ]
    copies.append(pltpu.make_async_copy(energy_ref, energy_hbm, sems.at[groups]))
    for copy in copies:
        copy.start()
    for copy in copies:
        copy.wait()


def spectra(starts, bins, weights, x, peers):
    n_var, n_time, n_pts = x.shape
    vmem, smem = pltpu.VMEM, pltpu.SMEM
    spec = pl.BlockSpec
    return pl.pallas_call(
        spectra_kernel,
        in_specs=[spec(memory_space=pl.ANY)] * 4,
        out_specs=[spec(memory_space=vmem)] * 4,
        out_shape=[
            vmem((peers, 1, QS * KF), jnp.float32),
            vmem((n_var, n_time, n_pts // 2), jnp.float32),
            vmem((n_var, n_time, n_pts // 2), jnp.float32),
            vmem((2 * NB, KF, n_time), jnp.float32),
        ],
        scratch_shapes=[
            vmem(x.shape, jnp.float32),
            smem(starts.shape, jnp.int32),
            vmem(bins.shape, jnp.int32),
            vmem(weights.shape, jnp.float32),
            vmem((n_var, 2 * NB * KF, n_pts), jnp.float32),
            vmem((QS, KF, n_pts), jnp.float32),
            pltpu.SemaphoreType.DMA((n_var + 3,)),
        ],
        name="spectra",
    )(starts, bins, weights, x)


def body(snapshots, weights, starts, bins):
    n_time, n_var, n_pts = snapshots.shape
    tiles = n_pts // LANES
    n_freq = lax.axis_size(FREQ)
    per_dev = bins.shape[0] // n_freq
    count = float(n_pts * n_freq * lax.axis_size(PTS) * n_var)
    gram, left, right, tab = spectra(
        starts, bins[None], weights[None], jnp.transpose(snapshots, (1, 0, 2)), 1
    )
    vmem = pltpu.VMEM
    keep = functools.partial(pltpu.with_memory_space_constraint, memory_space=vmem)
    in_vmem = pl.BlockSpec(memory_space=vmem)
    pairings = (("pts_1", 1), ("pts_0", 1), ("pts_0", 3))
    for step, (axis, flip) in enumerate(pairings, 1):
        other = lax.ppermute(gram, axis, [(i, i ^ flip) for i in range(lax.axis_size(axis))])
        gram = add(gram, other, n_freq if step == len(pairings) else 1)
    gram = lax.all_to_all(gram, FREQ, 0, 0, tiled=True)
    rows = 2 * n_var * tiles
    modes, energy = pl.pallas_call(
        functools.partial(modes_kernel, count),
        in_specs=[in_vmem] * 4,
        out_specs=[in_vmem] * 2,
        out_shape=[vmem((KF * rows, LANES), jnp.float32), vmem((1, per_dev), jnp.float32)],
        scratch_shapes=[vmem((3, n_var, n_time, n_pts), jnp.bfloat16)],
        name="modes",
    )(keep(gram), keep(tab), keep(left), keep(right))
    groups = per_dev * n_var
    modes = modes.reshape(n_freq, groups, 2 * tiles, LANES)
    modes = lax.all_to_all(modes, FREQ, 0, 0, tiled=True)
    modes, energy = pl.pallas_call(
        assemble_kernel,
        in_specs=[in_vmem] * 2,
        out_specs=[pl.BlockSpec(memory_space=pl.ANY)] * 2,
        out_shape=[
            jax.ShapeDtypeStruct((groups, n_freq, 2 * tiles, LANES), jnp.float32),
            jax.ShapeDtypeStruct((1, per_dev), jnp.float32),
        ],
        scratch_shapes=[pltpu.SemaphoreType.DMA((groups + 1,))],
        name="assemble",
    )(keep(modes), keep(energy))
    modes = modes.reshape(per_dev, n_var, n_freq * tiles, 2, LANES)
    modes = jnp.transpose(modes, (0, 3, 1, 2, 4)).reshape(per_dev, 2, n_var, n_freq * n_pts)
    return (modes, energy[0])


def solution(mesh):
    split = Mesh(mesh.devices.reshape(4, 8, 4, 2), ("freq_0", "freq_1", "pts_0", "pts_1"))
    placed = (P(None, None, PTS_FREQ), P(PTS_FREQ), P(), P())
    return jax.shard_map(
        body,
        mesh=split,
        in_specs=placed,
        out_specs=(P(FREQ, None, None, PTS), P(FREQ)),
        check_vma=False,
    )
```
